32 devices in a mesh: chan: 4 (over z), tm: 8 (over y, x, core).
Axes of the slice: x: 2, y: 2, z: 4, core: 2. Of those that a mesh axis runs over, the one named last changes fastest.
Arguments:
- trajectory: float32 [512, 8, 4096], P('tm', None, 'chan'), may hold values from -40 to 40
- initial: float32 [8, 4096], P(None, 'chan'), may hold values from -6 to 6
- drive_gate: bfloat16 [512, 8, 4096], P('tm', None, 'chan'), may hold values from -16 to 4
- drive_candidate: bfloat16 [512, 8, 4096], P('tm', None, 'chan'), may hold values from -6 to 6
- gate_weight: bfloat16 [4096, 4096], P('chan'), may hold values from -0.0234375 to 0.0234375
- candidate_weight: bfloat16 [4096, 4096], P('chan'), may hold values from -0.09375 to 0.09375
Outputs:
- newton_states: float32 [512, 8, 4096], P('tm', None, 'chan')
- residual_norm: float32 [], replicated
The draws below stay inside these ranges and needn't reach their ends.
All inputs are finite; a program needn't handle non-finite values.
Results may differ from the reference program's by a relative error of at most 0.0016.
Values may be sent and summed in bfloat16 or wider, within the bound.
A program may use at most 128 MiB of HBM per device.

```python
import jax
import jax.numpy as jnp
from jax import lax

H = 4096
BATCH = 8
TIME_STEP_COUNT = 512


def draw_trajectory(key, part):
    first_key = jax.random.fold_in(jax.random.fold_in(key, 11), 0)
    steps_frac = jnp.arange(TIME_STEP_COUNT, dtype=jnp.float32) / TIME_STEP_COUNT
    units_frac = jnp.arange(H, dtype=jnp.float32) / H
    growth = 0.5 * (4.0 ** steps_frac)[:, None, None] * (2.0 ** units_frac)[None, None, :]
    base = jnp.clip(jax.random.normal(first_key, (TIME_STEP_COUNT, BATCH, H), jnp.float32), -6.0, 6.0)
    values = base * growth
    return jnp.clip(values, -40.0, 40.0).astype(jnp.float32)


def draw_drive_gate(key, part):
    decay_random_key, jitter_random_key, spike_random_key = jax.random.split(jax.random.fold_in(key, 23), 3)
    log_rate = jax.random.uniform(decay_random_key, (H,), jnp.float32, jnp.log(1e-05), jnp.log(0.05))
    noise = 0.5 * jnp.clip(jax.random.normal(jitter_random_key, (TIME_STEP_COUNT, BATCH, H), jnp.float32), -4.0, 4.0)
    rate = jnp.exp(log_rate)
    spike_logits = jnp.log(rate) - jnp.log(1.0 - rate)
    spike_events = jax.random.randint(spike_random_key, (4,), 0, TIME_STEP_COUNT)
    step_values = jnp.arange(TIME_STEP_COUNT)
    spike_flags = jnp.any(step_values[:, None] == spike_events[None, :], axis=1)
    drive_level = jnp.where(spike_flags[:, None, None], -0.85, spike_logits[None, None, :])
    return jnp.clip(drive_level + noise, -16.0, 4.0).astype(jnp.bfloat16)


def shard_levels(stream_key, extent, shards, smallest, largest):
    loudness = 1.0
    for dim, blocks in shards:
        heights = jax.random.uniform(jax.random.fold_in(jax.random.fold_in(stream_key, 6), dim), (blocks,), jnp.float32, smallest / len(shards), largest / len(shards))
        loudness = loudness * jnp.repeat(jnp.exp(heights), extent[dim] // blocks).reshape((-1,) + (1,) * (len(extent) - 1 - dim))
    return loudness


def gaussian(key, dims, scale, most, cuts=(), kind=jnp.bfloat16):
    gain = shard_levels(key, dims, cuts, -0.22, 0.18) if cuts else 1.0
    entries = jax.random.normal(key, dims, jnp.float32) * scale * gain
    return jnp.minimum(jnp.maximum(entries, -most), most).astype(kind)


def setup_inputs(seed: int = 0) -> dict:
    key_list = jax.random.split(jax.random.key(seed), 7)
    return {
        "trajectory": draw_trajectory(jax.random.fold_in(key_list[6], 71), 0),
        "initial": gaussian(key_list[1], (BATCH, H), 1.0, 6.0, ((1, 4),), jnp.float32),
        "drive_gate": draw_drive_gate(jax.random.fold_in(key_list[6], 71), 0),
        "drive_candidate": gaussian(key_list[3], (TIME_STEP_COUNT, BATCH, H), 1.0, 6.0, ((0, 8), (2, 4))),
        "gate_weight": gaussian(key_list[4], (H, H), (16 * H) ** -0.5, 0.0234375, ((0, 4),)),
        "candidate_weight": gaussian(key_list[5], (H, H), H ** -0.5, 0.09375, ((0, 4),)),
    }


def advance(state, inputs):
    state = inputs[0] * state + inputs[1]
    return (state, state)

def reference(trajectory, initial, drive_gate, drive_candidate, gate_weight, candidate_weight):
    previous = jnp.concatenate([initial[None], trajectory[:-1]], 0)
    flat = previous.reshape(-1, H).astype(jnp.bfloat16)
    gate_pre = jnp.dot(flat, gate_weight, preferred_element_type=jnp.float32).reshape(previous.shape) + drive_gate.astype(jnp.float32)
    candidate_pre = jnp.dot(flat, candidate_weight, preferred_element_type=jnp.float32).reshape(previous.shape) + drive_candidate.astype(jnp.float32)
    gate_diagonal = jnp.diagonal(gate_weight).astype(jnp.float32)
    candidate_diagonal = jnp.diagonal(candidate_weight).astype(jnp.float32)
    update = jax.nn.sigmoid(gate_pre)
    candidate = jnp.tanh(candidate_pre)
    mapped = (1.0 - update) * previous + update * candidate
    jacobian = 1.0 - update + update * (1.0 - update) * (candidate - previous) * gate_diagonal + update * (1.0 - candidate * candidate) * candidate_diagonal
    offset = mapped - jacobian * previous
    _, newton_states = lax.scan(advance, initial, (jacobian, offset))
    missing = trajectory - mapped
    residual_norm = jnp.sqrt(jnp.mean(missing * missing) + 1e-06)
    return (newton_states, residual_norm)
```

```python
import functools

import jax
import jax.numpy as jnp
from jax import lax
from jax.experimental import pallas as pl
from jax.experimental.pallas import tpu as pltpu
from jax.sharding import PartitionSpec as P

MESH = pl.DeviceIdType.MESH
BF16 = jnp.bfloat16
F32 = jnp.float32

PACED = [0.0, 9.0, 13.65, 17.0]
FIRST = [10.0, 15.5, 20.5, 26.0]
FIRST_F = [13.5, 19.0, 27.0, 36.0]
FIRST_S = [18.0, 26.0, 34.5, 43.0]
AHEAD = 12.0
ROWS = [29.0, 36.5, 42.0, 50.0, 62.0, 70.0, 77.0, 83.0]
RELAY = [31.5, 39.5, 46.0, 54.0, 66.0, 73.5, 80.0, 85.0]
QUEUE = [34.0, 57.5, 64.0, 86.0]
SUMS = [47.0, 47.1, 56.9, 57.0, 75.9, 76.0, 84.5, 93.0]
GROUPS = [(0, 2), (2, 4), (4, 6), (6, 7), (7, 8)]
NEAR = [42.5, 60.0, 68.0, 92.0]
NEXT = [(8.0, 13.0), (4.0, 8.0), (7.0, 12.0), (1.5, 3.0)]
FAR = [45.5, 63.0]
NEXT_FAR = [(7.0, 12.0), (9.0, 15.0)]
LAST = [74.0, 75.0]
NEXT_LAST = [(7.0, 11.0), (8.0, 12.0)]
WHOLE = [72.0, 80.5, 81.0, 81.5]
ADDS = [76.5, 84.0, 90.0, 90.1]
ADDS_FAR = [65.0, 84.1]
FINAL = [[91.0, 91.1, 91.2, 98.0], [95.1, 95.2, 95.3, 98.1]]


def units_of(nz):
    near, far = (4, 2) if nz <= 4 else (1, 1)
    units = [(1, d, g, p, near) for p in range(near) for g in range(2) for d in range(1, nz - 1)]
    for d in range(1, nz - 1):
        pieces = near if d == 1 else far
        units += [(0, d, g, p, pieces) for p in range(pieces) for g in range(2)]
    if nz <= 4:
        units += [(0, nz - 1, g, p, near) for p in range(near // 2, near) for g in range(2)]
    return units


def split(count):
    rows = 1
    while rows * rows * 4 <= count:
        rows *= 2
    return rows, count // rows


def kernel(
    nz, nt, chunks, tile,
    traj_in, init, drive_g_in, drive_c_in, gate_w, cand_w,
    state, prod, entry_out, total,
    guess_buf, drive_g, drive_c, wbuf, abuf, acc, sbuf,
    diag, carry, ssq, partner_map, maps, tsums, zsums,
    load_sem, local_sem, wr_send, wr_recv, cr_send, cr_recv, wz_send, wz_recv, spread_send, f_recv, s_recv, c_recv,
    a_send, a_recv, sum_send, sum_recv, row_sem, pm_sem, m_send, m_recv, ts_send, ts_recv, zs_send, zs_recv,
):
    z = lax.axis_index("chan")
    t = lax.axis_index("tm")
    steps, batch, width = traj_in.shape
    nc = nt // 2
    na, nb = split(nc)
    chip = lax.div(t, 2)
    core = lax.rem(t, 2)
    chip_a = lax.div(chip, nb)
    chip_b = lax.rem(chip, nb)
    partner = (z, t + 1 - 2 * core)
    part = width // nt
    weights = (gate_w, cand_w)
    rows = steps * batch // chunks
    chunk_steps = steps // chunks
    half = nz // 2
    units = units_of(nz)
    index = {u[:4]: n for n, u in enumerate(units)}
    count = {u[:4]: u[4] for u in units}
    lower = z < half
    s = jnp.where(lower, 1, -1)
    is_end = jnp.logical_or(z == 0, z == nz - 1)
    is_inner = jnp.logical_not(is_end)
    beside_end = jnp.logical_or(z == 1, z == nz - 2)
    end = jnp.where(lower, 0, nz - 1)

    def remote(src, dst, send, recv, device):
        return pltpu.make_async_remote_copy(
            src_ref=src, dst_ref=dst, send_sem=send, recv_sem=recv,
            device_id=device, device_id_type=MESH,
        )

    def zmod(v):
        return lax.rem(v + 2 * nz, nz)

    def cmod(v):
        return lax.rem(v + 2 * nc, nc)

    def plane_cols(k):
        return pl.ds(pl.multiple_of(k * width, 128), width)

    def piece_cols(p, pieces):
        return pl.ds(p * (width // pieces), width // pieces)

    def chip_at(g, fast, slow):
        da, db = (slow, fast) if g == 0 else (fast, slow)
        return lax.rem(chip_a + da + na, na) * nb + lax.rem(chip_b + db + nb, nb)

    def extent(g):
        return (nb, na) if g == 0 else (na, nb)

    loads = [
        pltpu.make_async_copy(traj_in, guess_buf.at[pl.ds(1, steps)], load_sem.at[0]),
        pltpu.make_async_copy(drive_g_in, drive_g, load_sem.at[1]),
        pltpu.make_async_copy(drive_c_in, drive_c, load_sem.at[2]),
    ]
    for load in loads:
        load.start()

    barrier = pltpu.get_barrier_semaphore()
    for d in range(1, nz):
        pl.semaphore_signal(barrier, inc=1, device_id=(zmod(z + d), t), device_id_type=MESH)
    for d in range(1, nt):
        pl.semaphore_signal(barrier, inc=1, device_id=(z, lax.rem(t + d, nt)), device_id_type=MESH)
    pl.semaphore_wait(barrier, nz - 1 + nt - 1)

    def row_copy():
        return remote(
            traj_in.at[steps - 1], guess_buf.at[0], row_sem.at[0], row_sem.at[1], (z, lax.rem(t + 1, nt))
        )

    def w_slot(target, g, k, p, pieces, c):
        first = pl.multiple_of(k * width + (2 * c + core) * part, 16)
        return wbuf.at[target, g, pl.ds(first, part), piece_cols(p, pieces)]

    def w_send(unit, side, method):
        target, d, g, p = unit
        n, pieces = index[unit], count[unit]
        j = zmod(z - d) if side == 0 else zmod(z + d)
        if target == 1:
            valid = j == (1 if side == 0 else nz - 2)
            out = jnp.where(side == 0, 0, nz - 1)
        elif side == 0:
            valid = jnp.logical_and(j >= 1, j < half)
            out = j
        else:
            valid = jnp.logical_and(j >= half, j <= nz - 2)
            out = j

        @pl.when(valid)
        def _():
            step = width // pieces
            src = weights[g].at[
                pl.ds(pl.multiple_of(t * part, 16), part),
                pl.ds(pl.multiple_of(out * width + p * step, 128), step),
            ]
            copy = remote(
                src, w_slot(target, g, z, p, pieces, chip), wz_send.at[side % wz_send.shape[0], n], wz_recv.at[n], (j, t)
            )
            getattr(copy, method)()

    def w_pair(unit):
        def act(method):
            for side in range(2):
                w_send(unit, side, method)

        return act

    wholes = wr_recv.shape[0]
    whole_pieces = 4

    def whole_slot(g, k, p):
        return wbuf.at[0, g, plane_cols(k), piece_cols(p, whole_pieces)]

    def whole_pair(p):
        def act(method):
            for side in range(2):
                j = zmod(z + 1) if side == 0 else zmod(z - 1)
                valid = jnp.logical_and(j >= 1, j < half) if side == 0 else jnp.logical_and(j >= half, j <= nz - 2)
                step = width // whole_pieces
                for g in range(2):
                    @pl.when(jnp.logical_and(valid, core == g))
                    def _():
                        src = weights[g].at[:, pl.ds(pl.multiple_of(j * width + p * step, 128), step)]
                        copy = remote(src, whole_slot(g, z, p), wr_send.at[side, p], wr_recv.at[p], (j, t))
                        getattr(copy, method)()

        return act

    def run(entries, depth):
        for n, entry in enumerate(entries):
            if n >= depth:
                entries[n - depth]("wait_send")
            entry("start")
        for entry in entries[max(0, len(entries) - depth):]:
            entry("wait_send")

    row_copy().start()
    ahead = 4
    deep = 64
    first_units = [u[:4] for u in units if u[0] == 1]
    groups = max(u[3] for u in first_units) + 1

    def paced_weights(p):
        first_weights(p, p + 1)

    def first_weights(low, high):
        for u in first_units:
            if low <= u[3] < high:
                w_pair(u)("start")

    first_weights(0, 1)

    def own_copy(target, g):
        out = z if target == 0 else end
        return pltpu.make_async_copy(
            weights[g].at[:, plane_cols(out)],
            wbuf.at[target, g, plane_cols(z), :],
            local_sem.at[target, g],
        )

    for g in range(2):
        own_copy(0, g).start()

    @pl.when(is_inner)
    def _():
        for g in range(2):
            @pl.when(beside_end)
            def _():
                own_copy(1, g).start()

    for g in range(2):
        own_copy(0, g).wait()
        for j in range(width // 128):
            block = wbuf[0, g, pl.ds(pl.multiple_of(z * width + j * 128, 128), 128), pl.ds(j * 128, 128)]
            eye = lax.broadcasted_iota(jnp.int32, (128, 128), 0) == lax.broadcasted_iota(
                jnp.int32, (128, 128), 1
            )
            line = jnp.sum(jnp.where(eye, block.astype(F32), 0.0), axis=0, keepdims=True)
            diag[g, :, pl.ds(j * 128, 128)] = jnp.broadcast_to(line, (batch, 128))
    loads[0].wait()

    @pl.loop(1, steps // 2)
    def _(j):
        pair = guess_buf[pl.ds(2 * j, 2)].reshape(2 * batch, width)
        abuf[pl.ds(pl.multiple_of(j * 2 * batch, 16), 2 * batch), plane_cols(z)] = pair.astype(BF16)

    row_copy().wait()

    @pl.when(t == 0)
    def _():
        guess_buf[0] = init[...]

    abuf[pl.ds(0, 2 * batch), plane_cols(z)] = guess_buf[pl.ds(0, 2)].reshape(2 * batch, width).astype(BF16)

    def a_copy(way, m, i):
        k = z - s * m
        slot = abuf.at[pl.ds(i * rows, rows), plane_cols(k)]
        to = z + s if way == 0 else z - s
        return remote(slot, slot, a_send.at[way, min(abs(m), a_send.shape[1] - 1), i], a_recv.at[k, i], (to, t))

    def sum_copy(i):
        slot = sbuf.at[:, pl.ds(i * rows, rows), :]
        return remote(slot, slot, sum_send.at[i], sum_recv.at[i], (z - s, t))

    carry[0] = jnp.ones((batch, width), F32)
    carry[1] = jnp.zeros((batch, width), F32)
    ssq[...] = jnp.zeros((batch, width), F32)

    def local_products():
        @pl.loop(0, width // tile)
        def _(n):
            cols = pl.ds(pl.multiple_of(n * tile, tile), tile)
            for g in range(2):
                acc[g, :, cols] = jnp.dot(
                    abuf[:, plane_cols(z)], wbuf[0, g, plane_cols(z), cols], preferred_element_type=F32
                )

    def accumulate(d, low, high, first, last):
        k = zmod(z + s * d)
        span = pl.ds(low * rows, (high - low) * rows)

        @pl.loop(first, last)
        def _(n):
            cols = pl.ds(pl.multiple_of(n * tile, tile), tile)
            for g in range(2):
                acc[g, span, cols] += jnp.dot(
                    abuf[span, plane_cols(k)], wbuf[0, g, plane_cols(k), cols], preferred_element_type=F32
                )

    def gates(first, length, cols, wide, gate_pre, cand_pre):
        shape = (length, batch, wide)
        span = pl.ds(first, length)
        gate_pre = gate_pre.reshape(shape) + drive_g[span, :, cols].astype(F32)
        cand_pre = cand_pre.reshape(shape) + drive_c[span, :, cols].astype(F32)
        guess = guess_buf[pl.ds(first + 1, length), :, cols]
        previous = guess_buf[span, :, cols]
        update = jax.nn.sigmoid(gate_pre)
        candidate = jnp.tanh(cand_pre)
        keep = 1.0 - update
        mapped = keep * previous + update * candidate
        jacobian = (
            keep
            + update * keep * (candidate - previous) * diag[0, :, cols][None]
            + update * (1.0 - candidate * candidate) * diag[1, :, cols][None]
        )
        offset = mapped - jacobian * previous
        missing = guess - mapped
        ssq[:, cols] += jnp.sum(missing * missing, axis=0)
        product = carry[0, :, cols]
        value = carry[1, :, cols]
        for q in range(length):
            product = jacobian[q] * product
            value = jacobian[q] * value + offset[q]
            prod[first + q, :, cols] = product
            state[first + q, :, cols] = value
        carry[0, :, cols] = product
        carry[1, :, cols] = value

    final_pieces = count[(0, 1, 0, 0)]

    @pl.when(is_end)
    def _():
        def a_entry(i):
            return lambda method: getattr(a_copy(0, 0, i), method)()

        owns = [u[:4] for u in units if u[0] == 0 and half <= u[1] < nz - 1]
        lasts = [u[:4] for u in units if u[0] == 0 and u[1] == nz - 1]
        some = (len(owns) + 1) // 2
        whole = [whole_pair(p) for p in range(wholes)]
        local_products()
        for p in range(1, groups):
            paced_weights(p)
            for u in first_units:
                if u[3] == p - 1:
                    w_pair(u)("wait_send")
        run([a_entry(i) for i in range(chunks // 2)], ahead)
        run([w_pair(u) for u in owns[:some]], ahead)
        run([a_entry(i) for i in range(chunks // 2, chunks)], ahead)
        whole[0]("start")
        run([w_pair(u) for u in owns[some:] + lasts], ahead)
        for p in range(1, wholes):
            whole[p]("start")
        for p in range(wholes):
            whole[p]("wait_send")
        for u in first_units:
            if u[3] == groups - 1:
                w_pair(u)("wait_send")
        for load in loads[1:]:
            load.wait()
        for i in range(chunks):
            sum_copy(i).wait_recv()

            @pl.loop(0, width // tile)
            def _(n):
                cols = pl.ds(pl.multiple_of(n * tile, tile), tile)
                span = pl.ds(i * rows, rows)
                gates(
                    i * chunk_steps, chunk_steps, cols, tile,
                    acc[0, span, cols] + sbuf[0, span, cols].astype(F32),
                    acc[1, span, cols] + sbuf[1, span, cols].astype(F32),
                )

    def spread(unit, arrive, df, ds, device):
        target, d, g, p = unit
        n = index[unit]
        slot = w_slot(target, g, zmod(z + s * d), p, count[unit], chip_at(g, -df, -ds))
        return remote(slot, slot, spread_send.at[n], arrive.at[n], device)

    def f_copy(unit, df):
        return spread(unit, f_recv, 0, 0, (z, 2 * chip_at(unit[2], df, 0) + core))

    def s_copy(unit, df, ds):
        return spread(unit, s_recv, df, 0, (z, 2 * chip_at(unit[2], 0, ds) + core))

    def c_copy(unit, df, ds):
        return spread(unit, c_recv, df, ds, partner)

    def parts_of(unit, arrive, parts):
        target, d, g, p = unit
        n = index[unit]
        slot = wbuf.at[target, g, pl.ds(0, parts * part), piece_cols(p, count[unit])]
        return remote(slot, slot, spread_send.at[n], arrive.at[n], partner)

    def guarded(unit, body):
        if unit[0] == 1 and nz > 4:
            pl.when(beside_end)(body)
        else:
            body()

    def z_step(unit):
        def body():
            target, d, g, p = unit
            n = index[unit]
            nf, ns = extent(g)
            slot = w_slot(target, g, zmod(z + s * d), p, count[unit], chip)
            remote(slot, slot, wz_send.at[0, n], wz_recv.at[n], partner).wait_recv()
            for df in range(1, nf):
                f_copy(unit, df).start()
            for ds in range(1, ns):
                s_copy(unit, 0, ds).start()
            c_copy(unit, 0, 0).start()

        guarded(unit, body)

    def f_step(unit):
        def body():
            nf, ns = extent(unit[2])
            if nf > 1:
                parts_of(unit, f_recv, nf - 1).wait_recv()
            for df in range(1, nf):
                for ds in range(1, ns):
                    s_copy(unit, df, ds).start()
                c_copy(unit, df, 0).start()

        guarded(unit, body)

    def s_step(unit):
        def body():
            nf, ns = extent(unit[2])
            if ns > 1:
                parts_of(unit, s_recv, nf * (ns - 1)).wait_recv()
            for df in range(nf):
                for ds in range(1, ns):
                    c_copy(unit, df, ds).start()

        guarded(unit, body)

    def c_step(unit):
        def body():
            nf, ns = extent(unit[2])
            parts_of(unit, c_recv, nf * ns).wait_recv()

        guarded(unit, body)

    def all_sends(unit):
        def body():
            nf, ns = extent(unit[2])
            parts_of(unit, c_recv, nf - 1 + nf * (ns - 1) + nf * ns).wait_send()

        guarded(unit, body)

    def within(k):
        return jnp.logical_and(k >= 0, k < nz)

    outward = jnp.logical_and(z - s >= 1, z - s <= nz - 2)

    def need(m, i):
        @pl.when(within(z + s * m))
        def _():
            a_copy(0, -m, i).wait_recv()
            if nz > 4:
                @pl.when(outward)
                def _():
                    a_copy(1, -m, i).start()

    def partial_sums(low, high):
        def body():
            depth = (nz - 1) * width
            first = pl.multiple_of(jnp.where(lower, width, 0), 128)
            span = pl.ds(low * rows, (high - low) * rows)

            @pl.loop(0, width // tile)
            def _(n):
                cols = pl.ds(pl.multiple_of(n * tile, tile), tile)
                lhs = abuf[span, pl.ds(first, depth)]
                for g in range(2):
                    sbuf[g, span, cols] = jnp.dot(
                        lhs, wbuf[1, g, pl.ds(first, depth), cols], preferred_element_type=F32
                    ).astype(BF16)

            for i in range(low, high):
                sum_copy(i).start()

        if nz > 4:
            pl.when(beside_end)(body)
        else:
            body()

    def final(p, h):
        k = zmod(z + s)
        wide = width // final_pieces
        long = rows * 2

        @pl.loop(h * (chunks // 4), (h + 1) * (chunks // 4))
        def _(r):
            span = pl.ds(pl.multiple_of(r * long, long), long)
            for n in range(wide // min(tile, wide)):
                step = min(tile, wide)
                cols = pl.ds(p * wide + n * step, step)
                pre = [
                    acc[g, span, cols]
                    + jnp.dot(
                        abuf[span, plane_cols(k)], wbuf[0, g, plane_cols(k), cols], preferred_element_type=F32
                    )
                    for g in range(2)
                ]
                gates(r * (long // batch), long // batch, cols, step, *pre)

    def setup_end():
        def body():
            for g in range(2):
                own_copy(1, g).wait()

        if nz > 4:
            pl.when(beside_end)(body)
        else:
            body()

    def whole_step(p):
        k = zmod(z - s)
        for g in range(2):
            @pl.when(core == g)
            def _():
                slot = whole_slot(g, k, p)
                remote(slot, slot, wr_send.at[0, p], wr_recv.at[p], partner).wait_recv()
                remote(slot, slot, cr_send.at[p], cr_recv.at[p], partner).start()

    def whole_arrive(p):
        slot = whole_slot(0, zmod(z - s), p)
        remote(slot, slot, cr_send.at[p], cr_recv.at[p], partner).wait_recv()

    def whole_done(p):
        slot = whole_slot(0, zmod(z - s), p)
        remote(slot, slot, cr_send.at[p], cr_recv.at[p], partner).wait_send()

    events = []

    def at(time, body, *args):
        events.append((time, len(events), body, args))

    def w_entry(unit):
        return w_pair(unit)

    def rows_entry(i):
        def act(method):
            getattr(a_copy(0, 0, i), method)()
            if nz > 4:
                @pl.when(outward)
                def _():
                    getattr(a_copy(1, 0, i), method)()

        return act

    def relay_entry(m, i):
        def act(method):
            @pl.when(within(z - s * m))
            def _():
                if method == "start":
                    a_copy(0, m, i).wait_recv()
                getattr(a_copy(0, m, i), method)()

        return act

    queue = []

    def push(entry, done):
        queue.append((entry, done))

    def pump(n):
        if n >= deep:
            queue[n - deep][0]("wait_send")
        queue[n][0]("start")

    ends = [u[:4] for u in units if u[0] == 1]
    owns = [u[:4] for u in units if u[0] == 0]
    for u in ends:
        target, d, g, p = u
        e = 4 * p // groups if groups >= 4 else p
        at(FIRST[e] + 0.1 * d, z_step, u)
        at(FIRST_F[e] + 0.1 * d, f_step, u)
        at(FIRST_S[e] + 0.1 * d, s_step, u)
        at(SUMS[0] - 0.5, c_step, u)
        at(SUMS[0] + 10.0, all_sends, u)
    begun = 0
    for p in range(1, groups):
        at(PACED[p % 4], paced_weights, p)

    def last_paced():
        for u in first_units:
            w_pair(u)("wait_send")

    at(60.0, last_paced)
    for i in range(chunks):
        push(rows_entry(i), ROWS[i])
        for m in range(1, half):
            push(relay_entry(m, i), RELAY[i] + 0.01 * m)
        for m in range(1, nz - 1):
            at(SUMS[i] + 0.01 * m, need, m, i)
    for low, high in GROUPS:
        at(SUMS[high - 1] + 0.2, partial_sums, low, high)
    for u in owns:
        target, d, g, p = u
        if d == 1:
            push(w_entry(u), QUEUE[p] + 0.5 * g)
            done = NEAR[p] + 0.5 * g
        elif d == nz - 1:
            done = LAST[p - 2] + 0.5 * g
        else:
            done = FAR[p] + 3.0 * g + 0.1 * d
            if nz > 4:
                push(w_entry(u), 30.0 + 0.1 * d)
        after = NEXT[p] if d == 1 else NEXT_LAST[p - 2] if d == nz - 1 else NEXT_FAR[p]
        at(done, z_step, u)
        at(done + after[0], f_step, u)
        at(done + after[1], s_step, u)
        at(done + after[1] + (2.0 if done < 90.0 else 1.0), c_step, u)
    queue.sort(key=lambda entry: entry[1])
    previous_time = 0.0
    for n in range(begun, len(queue)):
        previous_time = max(previous_time + 0.001, queue[n][1] - AHEAD, 18.5)
        at(previous_time, pump, n)
    for p in range(wholes):
        at(WHOLE[p], whole_step, p)
        at(WHOLE[p] + 3.0, whole_arrive, p)

    tiles = width // tile
    if nz > 4:
        for p in range(wholes):
            at(26.0, whole_pair(p), "start")
    at(4.0, local_products)
    at(4.1, setup_end)
    if nz == 4:
        middle = chunks // 2
        for h in range(2):
            at(ADDS_FAR[h], accumulate, 2, 0, middle, h * tiles // 2, (h + 1) * tiles // 2)
        at(SUMS[7] + 1.0, accumulate, 2, middle, chunks, 0, tiles)
        for p in range(4):
            at(ADDS[p], accumulate, 3, 0, chunks, p * tiles // 4, (p + 1) * tiles // 4)
    else:
        for d in range(2, nz):
            at(98.0 + 0.1 * d, accumulate, d, 0, chunks, 0, tiles)
    for load in loads[1:]:
        at(20.0, load.wait)
    for p in range(final_pieces):
        for h in range(2):
            at(FINAL[h][p] if nz == 4 else 99.0 + 0.1 * h + 0.01 * p, final, p, h)

    @pl.when(is_inner)
    def _():
        for _, _, body, args in sorted(events, key=lambda event: event[:2]):
            body(*args)

    def pm_copy():
        return remote(carry, partner_map, pm_sem.at[0], pm_sem.at[1], partner)

    pm_copy().start()
    mine = ssq[:, pl.ds(0, 128)]
    for j in range(1, width // 128):
        mine = mine + ssq[:, pl.ds(j * 128, 128)]
    tsums[t] = mine

    def ts_copy(d):
        slot = tsums.at[t]
        return remote(slot, slot, ts_send.at[d - 1], ts_recv.at[d - 1], (z, lax.rem(t + d, nt)))

    def ts_arrival(d):
        slot = tsums.at[lax.rem(t + nt - d, nt)]
        return remote(slot, slot, ts_send.at[d - 1], ts_recv.at[d - 1], partner)

    for d in range(1, nt):
        ts_copy(d).start()

    def m_copy(dq):
        slot = maps.at[chip]
        return remote(
            slot, slot, m_send.at[dq - 1], m_recv.at[dq - 1], (z, 2 * cmod(chip + dq) + core)
        )

    def m_arrival(dq):
        slot = maps.at[cmod(chip - dq)]
        return remote(slot, slot, m_send.at[dq - 1], m_recv.at[dq - 1], partner)

    pm_copy().wait()
    is_second = core == 1
    p_mine, s_mine, p_other, s_other = carry[0], carry[1], partner_map[0], partner_map[1]
    p_late = jnp.where(is_second, p_mine, p_other)
    s_early = jnp.where(is_second, s_other, s_mine)
    s_late = jnp.where(is_second, s_mine, s_other)
    maps[chip, 0] = p_mine * p_other
    maps[chip, 1] = p_late * s_early + s_late
    for dq in range(1, nc):
        m_copy(dq).start()

    @pl.when(is_inner)
    def _():
        for u in owns:
            all_sends(u)
        for entry, _ in queue[max(0, len(queue) - deep):]:
            entry("wait_send")
        for p in range(wholes):
            whole_done(p)
            if nz > 4:
                whole_pair(p)("wait_send")
        for i in range(chunks):
            if nz > 4:
                @pl.when(outward)
                def _():
                    for m in range(1, nz - 1):
                        @pl.when(within(z + s * m))
                        def _():
                            a_copy(1, -m, i).wait_send()

            @pl.when(beside_end)
            def _():
                sum_copy(i).wait_send()

    for d in range(1, nt):
        ts_arrival(d).wait_recv()
    plane = tsums[0]
    for k in range(1, nt):
        plane = plane + tsums[k]
    zsums[z] = plane

    def zs_copy(d):
        slot = zsums.at[z]
        return remote(slot, slot, zs_send.at[d - 1], zs_recv.at[d - 1], (zmod(z + d), t))

    def zs_arrival(d):
        slot = zsums.at[zmod(z - d)]
        return remote(slot, slot, zs_send.at[d - 1], zs_recv.at[d - 1], partner)

    for d in range(1, nz):
        zs_copy(d).start()

    for dq in range(1, nc):
        m_arrival(dq).wait_recv()
    entry = init[...]
    for q in range(nc):
        entry = jnp.where(q < chip, maps[q, 0] * entry + maps[q, 1], entry)
    entry_out[...] = jnp.where(is_second, p_other * entry + s_other, entry)

    for d in range(1, nt):
        ts_copy(d).wait_send()
    for dq in range(1, nc):
        m_copy(dq).wait_send()
    for d in range(1, nz):
        zs_arrival(d).wait_recv()
    whole = zsums[0]
    for k in range(1, nz):
        whole = whole + zsums[k]
    total[...] = whole
    for d in range(1, nz):
        zs_copy(d).wait_send()


def finish(entries, state, prod, entry, total, states, norm, held, out_sem):
    parts = out_sem.shape[0]
    span = state.shape[0] // parts

    def put(n):
        return pltpu.make_async_copy(
            held.at[pl.ds(n * span, span)], states.at[pl.ds(n * span, span)], out_sem.at[n]
        )

    for n in range(parts):
        @pl.loop(n * span, (n + 1) * span)
        def _(q):
            held[q] = prod[q] * entry[...] + state[q]

        put(n).start()
    line = jnp.sum(total[...], axis=0, keepdims=True)
    norm[...] = jnp.sqrt(jnp.sum(line, axis=1, keepdims=True) / entries + 1e-06)
    for n in range(parts):
        put(n).wait()


def local(nz, nt, trajectory, initial, drive_gate, drive_candidate, gate_weight, candidate_weight):
    steps, batch, width = trajectory.shape
    nc = nt // 2
    full = gate_weight.shape[1]
    chunks = 8
    parts = 8
    tile = min(256, width)
    units = len(units_of(nz))
    pieces = 2 if nz == 4 else 4
    ways = 1 if nz == 4 else 2
    entries = trajectory.size * nz * nt
    dma = pltpu.SemaphoreType.DMA
    vmem = pl.BlockSpec(memory_space=pltpu.VMEM)
    hbm = pl.BlockSpec(memory_space=pltpu.HBM)
    block = (steps, batch, width)
    state, prod, entry, total = pl.pallas_call(
        functools.partial(kernel, nz, nt, chunks, tile),
        out_shape=(
            pltpu.VMEM(block, F32),
            pltpu.VMEM(block, F32),
            pltpu.VMEM((batch, width), F32),
            pltpu.VMEM((batch, 128), F32),
        ),
        in_specs=[hbm, vmem, hbm, hbm, hbm, hbm],
        out_specs=(vmem, vmem, vmem, vmem),
        scratch_shapes=[
            pltpu.VMEM((steps + 1, batch, width), F32),
            pltpu.VMEM(block, BF16),
            pltpu.VMEM(block, BF16),
            pltpu.VMEM((2, 2, full, width), BF16),
            pltpu.VMEM((steps * batch, full), BF16),
            pltpu.VMEM((2, steps * batch, width), F32),
            pltpu.VMEM((2, steps * batch, width), BF16),
            pltpu.VMEM((2, batch, width), F32),
            pltpu.VMEM((2, batch, width), F32),
            pltpu.VMEM((batch, width), F32),
            pltpu.VMEM((2, batch, width), F32),
            pltpu.VMEM((nc, 2, batch, width), F32),
            pltpu.VMEM((nt, batch, 128), F32),
            pltpu.VMEM((nz, batch, 128), F32),
            dma((3,)),
            dma((2, 2)),
            dma((2, pieces)),
            dma((pieces,)),
            dma((pieces,)),
            dma((pieces,)),
            dma((ways, units)),
            dma((units,)),
            dma((units,)),
            dma((units,)),
            dma((units,)),
            dma((units,)),
            dma((ways, nz // 2 if ways == 1 else nz, chunks)),
            dma((nz, chunks)),
            dma((chunks,)),
            dma((chunks,)),
            dma((2,)),
            dma((2,)),
            dma((nc - 1,)),
            dma((nc - 1,)),
            dma((nt - 1,)),
            dma((nt - 1,)),
            dma((nz - 1,)),
            dma((nz - 1,)),
        ],
        compiler_params=pltpu.CompilerParams(
            collective_id=0, has_side_effects=True, vmem_limit_bytes=56 * 2**20
        ),
    )(*(
        pltpu.with_memory_space_constraint(x, pltpu.HBM) if x.ndim == 3 or x.shape[1] == full else x
        for x in (trajectory, initial, drive_gate, drive_candidate, gate_weight, candidate_weight)
    ))
    states, norm = pl.pallas_call(
        functools.partial(finish, entries),
        out_shape=(jax.ShapeDtypeStruct(block, F32), jax.ShapeDtypeStruct((1, 1), F32)),
        in_specs=[vmem, vmem, vmem, vmem],
        out_specs=(hbm, vmem),
        scratch_shapes=[pltpu.VMEM(block, F32), dma((parts,))],
        compiler_params=pltpu.CompilerParams(vmem_limit_bytes=8 * 2**20),
    )(state, prod, entry, total)
    return (states, norm.reshape(()))


def solution(mesh):
    placed = (
        P("tm", None, "chan"),
        P(None, "chan"),
        P("tm", None, "chan"),
        P("tm", None, "chan"),
        P("chan", None),
        P("chan", None),
    )
    body = functools.partial(local, mesh.shape["chan"], mesh.shape["tm"])
    return jax.shard_map(
        body, mesh=mesh, in_specs=placed, out_specs=(P("tm", None, "chan"), P()), check_vma=False
    )
```

```python
import functools

import jax
import jax.numpy as jnp
from jax import lax
from jax.experimental import pallas as pl
from jax.experimental.pallas import tpu as pltpu
from jax.sharding import PartitionSpec as P

MESH = pl.DeviceIdType.MESH
BF16 = jnp.bfloat16
F32 = jnp.float32

PACED = [0.0, 9.0, 13.65, 17.0]
FIRST = [10.0, 15.5, 20.5, 26.0]
FIRST_F = [13.5, 19.0, 27.0, 36.0]
FIRST_S = [18.0, 26.0, 34.5, 43.0]
LOCAL = [25.5, 34.4, 36.5, 42.9]
AHEAD = 12.0
ROWS = [28.0, 36.0, 40.0, 48.0, 59.0, 64.0, 72.0, 78.0]
RELAY = [30.5, 38.0, 43.0, 51.0, 61.5, 66.0, 75.0, 81.0]
QUEUE = [33.0, 46.0, 68.0, 77.0]
SUMS = [47.0, 47.1, 58.5, 66.5, 71.5, 77.5, 84.0, 90.0]
GROUPS = [(0, 2), (2, 3), (3, 4), (4, 5), (5, 6), (6, 7), (7, 8)]
NEAR = [42.5, 53.0, 74.0, 86.0]
NEXT = [(8.0, 12.0), (8.0, 12.0), (6.5, 11.0), (4.5, 7.5)]
FAR = [45.5, 63.0]
NEXT_FAR = [(9.0, 14.5), (6.0, 12.0)]
LAST = [71.0]
NEXT_LAST = [(7.0, 12.5)]
WHOLE = [70.5, 77.5, 87.6, 88.0]
ADDS = [74.0, 81.0, 91.0, 88.6]
SPANS = [(0, 4), (4, 6), (6, 8)]
FINAL = [[74.2, 81.1, 91.1, 96.2], [81.2, 81.3, 91.2, 96.3], [92.0, 92.4, 92.5, 96.4]]


def units_of(nz):
    near, far = (4, 2) if nz <= 4 else (1, 1)
    units = [(1, d, g, p, near) for p in range(near) for g in range(2) for d in range(1, nz - 1)]
    for d in range(1, nz - 1):
        pieces = near if d == 1 else far
        units += [(0, d, g, p, pieces) for p in range(pieces) for g in range(2)]
    if nz <= 4:
        units += [(0, nz - 1, g, p, near) for p in range(near - 1, near) for g in range(2)]
    return units


def split(count):
    rows = 1
    while rows * rows * 4 <= count:
        rows *= 2
    return rows, count // rows


def kernel(
    nz, nt, chunks, tile,
    traj_in, init, drive_g_in, drive_c_in, gate_w, cand_w,
    state, prod, entry_out, total,
    guess_buf, drive_g, drive_c, wbuf, abuf, acc, end_acc, sbuf,
    diag, carry, ssq, partner_map, maps, tsums, zsums,
    load_sem, local_sem, wr_send, wr_recv, cr_send, cr_recv, wz_send, wz_recv, spread_send, f_recv, s_recv, c_recv,
    a_send, a_recv, sum_send, sum_recv, row_sem, pm_sem, m_send, m_recv, ts_send, ts_recv, zs_send, zs_recv,
):
    z = lax.axis_index("chan")
    t = lax.axis_index("tm")
    steps, batch, width = traj_in.shape
    nc = nt // 2
    na, nb = split(nc)
    chip = lax.div(t, 2)
    core = lax.rem(t, 2)
    chip_a = lax.div(chip, nb)
    chip_b = lax.rem(chip, nb)
    partner = (z, t + 1 - 2 * core)
    part = width // nt
    weights = (gate_w, cand_w)
    rows = steps * batch // chunks
    chunk_steps = steps // chunks
    half = nz // 2
    units = units_of(nz)
    index = {u[:4]: n for n, u in enumerate(units)}
    count = {u[:4]: u[4] for u in units}
    lower = z < half
    s = jnp.where(lower, 1, -1)
    is_end = jnp.logical_or(z == 0, z == nz - 1)
    is_inner = jnp.logical_not(is_end)
    beside_end = jnp.logical_or(z == 1, z == nz - 2)
    end = jnp.where(lower, 0, nz - 1)

    def remote(src, dst, send, recv, device):
        return pltpu.make_async_remote_copy(
            src_ref=src, dst_ref=dst, send_sem=send, recv_sem=recv,
            device_id=device, device_id_type=MESH,
        )

    def zmod(v):
        return lax.rem(v + 2 * nz, nz)

    def cmod(v):
        return lax.rem(v + 2 * nc, nc)

    def plane_cols(k):
        return pl.ds(pl.multiple_of(k * width, 128), width)

    def piece_cols(p, pieces):
        return pl.ds(p * (width // pieces), width // pieces)

    def chip_at(g, fast, slow):
        da, db = (slow, fast) if g == 0 else (fast, slow)
        return lax.rem(chip_a + da + na, na) * nb + lax.rem(chip_b + db + nb, nb)

    def extent(g):
        return (nb, na) if g == 0 else (na, nb)

    loads = [
        pltpu.make_async_copy(traj_in, guess_buf.at[pl.ds(1, steps)], load_sem.at[0]),
        pltpu.make_async_copy(drive_g_in, drive_g, load_sem.at[1]),
        pltpu.make_async_copy(drive_c_in, drive_c, load_sem.at[2]),
    ]
    for load in loads:
        load.start()

    barrier = pltpu.get_barrier_semaphore()
    for d in range(1, nz):
        pl.semaphore_signal(barrier, inc=1, device_id=(zmod(z + d), t), device_id_type=MESH)
    for d in range(1, nt):
        pl.semaphore_signal(barrier, inc=1, device_id=(z, lax.rem(t + d, nt)), device_id_type=MESH)
    pl.semaphore_wait(barrier, nz - 1 + nt - 1)

    def row_copy():
        return remote(
            traj_in.at[steps - 1], guess_buf.at[0], row_sem.at[0], row_sem.at[1], (z, lax.rem(t + 1, nt))
        )

    def w_slot(target, g, k, p, pieces, c):
        first = pl.multiple_of(k * width + (2 * c + core) * part, 16)
        return wbuf.at[target, g, pl.ds(first, part), piece_cols(p, pieces)]

    def w_send(unit, side, method):
        target, d, g, p = unit
        n, pieces = index[unit], count[unit]
        j = zmod(z - d) if side == 0 else zmod(z + d)
        if target == 1:
            valid = j == (1 if side == 0 else nz - 2)
            out = jnp.where(side == 0, 0, nz - 1)
        elif side == 0:
            valid = jnp.logical_and(j >= 1, j < half)
            out = j
        else:
            valid = jnp.logical_and(j >= half, j <= nz - 2)
            out = j

        @pl.when(valid)
        def _():
            step = width // pieces
            src = weights[g].at[
                pl.ds(pl.multiple_of(t * part, 16), part),
                pl.ds(pl.multiple_of(out * width + p * step, 128), step),
            ]
            copy = remote(
                src, w_slot(target, g, z, p, pieces, chip), wz_send.at[side % wz_send.shape[0], n], wz_recv.at[n], (j, t)
            )
            getattr(copy, method)()

    def w_pair(unit):
        def act(method):
            for side in range(2):
                w_send(unit, side, method)

        return act

    wholes = wr_recv.shape[0]
    whole_pieces = 4

    def whole_slot(g, k, p):
        return wbuf.at[0, g, plane_cols(k), piece_cols(p, whole_pieces)]

    def whole_pair(p):
        def act(method):
            for side in range(2):
                j = zmod(z + 1) if side == 0 else zmod(z - 1)
                valid = jnp.logical_and(j >= 1, j < half) if side == 0 else jnp.logical_and(j >= half, j <= nz - 2)
                step = width // whole_pieces
                for g in range(2):
                    @pl.when(jnp.logical_and(valid, core == g))
                    def _():
                        src = weights[g].at[:, pl.ds(pl.multiple_of(j * width + p * step, 128), step)]
                        copy = remote(src, whole_slot(g, z, p), wr_send.at[side, p], wr_recv.at[p], (j, t))
                        getattr(copy, method)()

        return act

    def run(entries, depth):
        for n, entry in enumerate(entries):
            if n >= depth:
                entries[n - depth]("wait_send")
            entry("start")
        for entry in entries[max(0, len(entries) - depth):]:
            entry("wait_send")

    row_copy().start()
    ahead = 4
    deep = 64
    first_units = [u[:4] for u in units if u[0] == 1]
    groups = max(u[3] for u in first_units) + 1

    def paced_weights(p):
        first_weights(p, p + 1)

    def first_weights(low, high):
        for u in first_units:
            if low <= u[3] < high:
                w_pair(u)("start")

    first_weights(0, 1)

    def own_copy(target, g):
        out = z if target == 0 else end
        return pltpu.make_async_copy(
            weights[g].at[:, plane_cols(out)],
            wbuf.at[target, g, plane_cols(z), :],
            local_sem.at[target, g],
        )

    for g in range(2):
        own_copy(0, g).start()

    @pl.when(is_inner)
    def _():
        for g in range(2):
            @pl.when(beside_end)
            def _():
                own_copy(1, g).start()

    for g in range(2):
        own_copy(0, g).wait()
        for j in range(width // 128):
            block = wbuf[0, g, pl.ds(pl.multiple_of(z * width + j * 128, 128), 128), pl.ds(j * 128, 128)]
            eye = lax.broadcasted_iota(jnp.int32, (128, 128), 0) == lax.broadcasted_iota(
                jnp.int32, (128, 128), 1
            )
            line = jnp.sum(jnp.where(eye, block.astype(F32), 0.0), axis=0, keepdims=True)
            diag[g, :, pl.ds(j * 128, 128)] = jnp.broadcast_to(line, (batch, 128))
    loads[0].wait()

    @pl.loop(1, steps // 2)
    def _(j):
        pair = guess_buf[pl.ds(2 * j, 2)].reshape(2 * batch, width)
        abuf[pl.ds(pl.multiple_of(j * 2 * batch, 16), 2 * batch), plane_cols(z)] = pair.astype(BF16)

    row_copy().wait()

    @pl.when(t == 0)
    def _():
        guess_buf[0] = init[...]

    abuf[pl.ds(0, 2 * batch), plane_cols(z)] = guess_buf[pl.ds(0, 2)].reshape(2 * batch, width).astype(BF16)

    def a_copy(way, m, i):
        k = z - s * m
        slot = abuf.at[pl.ds(i * rows, rows), plane_cols(k)]
        to = z + s if way == 0 else z - s
        return remote(slot, slot, a_send.at[way, min(abs(m), a_send.shape[1] - 1), i], a_recv.at[k, i], (to, t))

    def sum_copy(i):
        slot = sbuf.at[:, pl.ds(i * rows, rows), :]
        return remote(slot, slot, sum_send.at[i], sum_recv.at[i], (z - s, t))

    carry[0] = jnp.ones((batch, width), F32)
    carry[1] = jnp.zeros((batch, width), F32)
    ssq[...] = jnp.zeros((batch, width), F32)

    def local_products():
        @pl.loop(0, width // tile)
        def _(n):
            cols = pl.ds(pl.multiple_of(n * tile, tile), tile)
            for g in range(2):
                acc[g, :, cols] = jnp.dot(
                    abuf[:, plane_cols(z)], wbuf[0, g, plane_cols(z), cols], preferred_element_type=F32
                )

    def accumulate(d, low, high, first, last):
        k = zmod(z + s * d)
        span = pl.ds(low * rows, (high - low) * rows)

        @pl.loop(first, last)
        def _(n):
            cols = pl.ds(pl.multiple_of(n * tile, tile), tile)
            for g in range(2):
                acc[g, span, cols] += jnp.dot(
                    abuf[span, plane_cols(k)], wbuf[0, g, plane_cols(k), cols], preferred_element_type=F32
                )

    def gates(first, length, cols, wide, gate_pre, cand_pre):
        shape = (length, batch, wide)
        span = pl.ds(first, length)
        gate_pre = gate_pre.reshape(shape) + drive_g[span, :, cols].astype(F32)
        cand_pre = cand_pre.reshape(shape) + drive_c[span, :, cols].astype(F32)
        guess = guess_buf[pl.ds(first + 1, length), :, cols]
        previous = guess_buf[span, :, cols]
        update = jax.nn.sigmoid(gate_pre)
        candidate = jnp.tanh(cand_pre)
        keep = 1.0 - update
        mapped = keep * previous + update * candidate
        jacobian = (
            keep
            + update * keep * (candidate - previous) * diag[0, :, cols][None]
            + update * (1.0 - candidate * candidate) * diag[1, :, cols][None]
        )
        offset = mapped - jacobian * previous
        missing = guess - mapped
        ssq[:, cols] += jnp.sum(missing * missing, axis=0)
        product = carry[0, :, cols]
        value = carry[1, :, cols]
        for q in range(length):
            product = jacobian[q] * product
            value = jacobian[q] * value + offset[q]
            prod[first + q, :, cols] = product
            state[first + q, :, cols] = value
        carry[0, :, cols] = product
        carry[1, :, cols] = value

    final_pieces = count[(0, 1, 0, 0)]

    @pl.when(is_end)
    def _():
        def a_entry(i):
            return lambda method: getattr(a_copy(0, 0, i), method)()

        owns = [u[:4] for u in units if u[0] == 0 and half <= u[1] < nz - 1]
        lasts = [u[:4] for u in units if u[0] == 0 and u[1] == nz - 1]
        some = (len(owns) + 1) // 2
        whole = [whole_pair(p) for p in range(wholes)]
        local_products()
        for p in range(1, groups):
            paced_weights(p)
            for u in first_units:
                if u[3] == p - 1:
                    w_pair(u)("wait_send")
        run([a_entry(i) for i in range(chunks // 2)], ahead)
        run([w_pair(u) for u in owns[:some]], ahead)
        run([a_entry(i) for i in range(chunks // 2, chunks)], ahead)
        whole[0]("start")
        run([w_pair(u) for u in owns[some:] + lasts], ahead)
        for p in range(1, wholes):
            whole[p]("start")
        for p in range(wholes):
            whole[p]("wait_send")
        for u in first_units:
            if u[3] == groups - 1:
                w_pair(u)("wait_send")
        for load in loads[1:]:
            load.wait()
        for i in range(chunks):
            sum_copy(i).wait_recv()

            @pl.loop(0, width // tile)
            def _(n):
                cols = pl.ds(pl.multiple_of(n * tile, tile), tile)
                span = pl.ds(i * rows, rows)
                gates(
                    i * chunk_steps, chunk_steps, cols, tile,
                    acc[0, span, cols] + sbuf[0, span, cols].astype(F32),
                    acc[1, span, cols] + sbuf[1, span, cols].astype(F32),
                )

    def spread(unit, arrive, df, ds, device):
        target, d, g, p = unit
        n = index[unit]
        slot = w_slot(target, g, zmod(z + s * d), p, count[unit], chip_at(g, -df, -ds))
        return remote(slot, slot, spread_send.at[n], arrive.at[n], device)

    def f_copy(unit, df):
        return spread(unit, f_recv, 0, 0, (z, 2 * chip_at(unit[2], df, 0) + core))

    def s_copy(unit, df, ds):
        return spread(unit, s_recv, df, 0, (z, 2 * chip_at(unit[2], 0, ds) + core))

    def c_copy(unit, df, ds):
        return spread(unit, c_recv, df, ds, partner)

    def parts_of(unit, arrive, parts):
        target, d, g, p = unit
        n = index[unit]
        slot = wbuf.at[target, g, pl.ds(0, parts * part), piece_cols(p, count[unit])]
        return remote(slot, slot, spread_send.at[n], arrive.at[n], partner)

    def guarded(unit, body):
        if unit[0] == 1 and nz > 4:
            pl.when(beside_end)(body)
        else:
            body()

    def z_step(unit):
        def body():
            target, d, g, p = unit
            n = index[unit]
            nf, ns = extent(g)
            slot = w_slot(target, g, zmod(z + s * d), p, count[unit], chip)
            remote(slot, slot, wz_send.at[0, n], wz_recv.at[n], partner).wait_recv()
            for df in range(1, nf):
                f_copy(unit, df).start()
            for ds in range(1, ns):
                s_copy(unit, 0, ds).start()
            c_copy(unit, 0, 0).start()

        guarded(unit, body)

    def f_step(unit):
        def body():
            nf, ns = extent(unit[2])
            if nf > 1:
                parts_of(unit, f_recv, nf - 1).wait_recv()
            for df in range(1, nf):
                for ds in range(1, ns):
                    s_copy(unit, df, ds).start()
                c_copy(unit, df, 0).start()

        guarded(unit, body)

    def s_step(unit):
        def body():
            nf, ns = extent(unit[2])
            if ns > 1:
                parts_of(unit, s_recv, nf * (ns - 1)).wait_recv()
            for df in range(nf):
                for ds in range(1, ns):
                    c_copy(unit, df, ds).start()

        guarded(unit, body)

    def c_step(unit):
        def body():
            nf, ns = extent(unit[2])
            parts_of(unit, c_recv, nf * ns).wait_recv()

        guarded(unit, body)

    def all_sends(unit):
        def body():
            nf, ns = extent(unit[2])
            parts_of(unit, c_recv, nf - 1 + nf * (ns - 1) + nf * ns).wait_send()

        guarded(unit, body)

    def within(k):
        return jnp.logical_and(k >= 0, k < nz)

    outward = jnp.logical_and(z - s >= 1, z - s <= nz - 2)

    def need(m, i):
        @pl.when(within(z + s * m))
        def _():
            a_copy(0, -m, i).wait_recv()
            if nz > 4:
                @pl.when(outward)
                def _():
                    a_copy(1, -m, i).start()

    def local_sums(first, last):
        def body():
            @pl.loop(first, last)
            def _(n):
                cols = pl.ds(pl.multiple_of(n * tile, tile), tile)
                for g in range(2):
                    end_acc[g, :, cols] = jnp.dot(
                        abuf[:, plane_cols(z)], wbuf[1, g, plane_cols(z), cols], preferred_element_type=F32
                    )

        if nz > 4:
            pl.when(beside_end)(body)
        else:
            body()

    def partial_sums(low, high):
        def body():
            depth = (nz - 2) * width
            first = pl.multiple_of(jnp.where(lower, 2 * width, 0), 128)
            span = pl.ds(low * rows, (high - low) * rows)

            @pl.loop(0, width // tile)
            def _(n):
                cols = pl.ds(pl.multiple_of(n * tile, tile), tile)
                lhs = abuf[span, pl.ds(first, depth)]
                for g in range(2):
                    sbuf[g, span, cols] = (
                        end_acc[g, span, cols]
                        + jnp.dot(lhs, wbuf[1, g, pl.ds(first, depth), cols], preferred_element_type=F32)
                    ).astype(BF16)

            for i in range(low, high):
                sum_copy(i).start()

        if nz > 4:
            pl.when(beside_end)(body)
        else:
            body()

    def final(p, low, high):
        blocks = [zmod(z + s * d) for d in ((1, 2) if nz == 4 else (1,))]
        wide = width // final_pieces
        long = rows * 2

        @pl.loop(low // 2, high // 2)
        def _(r):
            span = pl.ds(pl.multiple_of(r * long, long), long)
            for n in range(wide // min(tile, wide)):
                step = min(tile, wide)
                cols = pl.ds(p * wide + n * step, step)
                pre = []
                for g in range(2):
                    sums = acc[g, span, cols]
                    for k in blocks:
                        sums += jnp.dot(
                            abuf[span, plane_cols(k)], wbuf[0, g, plane_cols(k), cols],
                            preferred_element_type=F32,
                        )
                    pre.append(sums)
                gates(r * (long // batch), long // batch, cols, step, *pre)

    def setup_end():
        def body():
            for g in range(2):
                own_copy(1, g).wait()

        if nz > 4:
            pl.when(beside_end)(body)
        else:
            body()

    def whole_step(p):
        k = zmod(z - s)
        for g in range(2):
            @pl.when(core == g)
            def _():
                slot = whole_slot(g, k, p)
                remote(slot, slot, wr_send.at[0, p], wr_recv.at[p], partner).wait_recv()
                remote(slot, slot, cr_send.at[p], cr_recv.at[p], partner).start()

    def whole_arrive(p):
        slot = whole_slot(0, zmod(z - s), p)
        remote(slot, slot, cr_send.at[p], cr_recv.at[p], partner).wait_recv()

    def whole_done(p):
        slot = whole_slot(0, zmod(z - s), p)
        remote(slot, slot, cr_send.at[p], cr_recv.at[p], partner).wait_send()

    events = []

    def at(time, body, *args):
        events.append((time, len(events), body, args))

    def w_entry(unit):
        return w_pair(unit)

    def rows_entry(i):
        def act(method):
            getattr(a_copy(0, 0, i), method)()
            if nz > 4:
                @pl.when(outward)
                def _():
                    getattr(a_copy(1, 0, i), method)()

        return act

    def relay_entry(m, i):
        def act(method):
            @pl.when(within(z - s * m))
            def _():
                if method == "start":
                    a_copy(0, m, i).wait_recv()
                getattr(a_copy(0, m, i), method)()

        return act

    queue = []

    def push(entry, done):
        queue.append((entry, done))

    def pump(n):
        if n >= deep:
            queue[n - deep][0]("wait_send")
        queue[n][0]("start")

    ends = [u[:4] for u in units if u[0] == 1]
    owns = [u[:4] for u in units if u[0] == 0]
    for u in ends:
        target, d, g, p = u
        e = 4 * p // groups if groups >= 4 else p
        at(FIRST[e] + 0.1 * d, z_step, u)
        at(FIRST_F[e] + 0.1 * d, f_step, u)
        at(FIRST_S[e] + 0.1 * d, s_step, u)
        at(SUMS[0] - 0.5, c_step, u)
        at(SUMS[0] + 10.0, all_sends, u)
    begun = 0
    for p in range(1, groups):
        at(PACED[p % 4], paced_weights, p)

    def last_paced():
        for u in first_units:
            w_pair(u)("wait_send")

    at(60.0, last_paced)
    for i in range(chunks):
        push(rows_entry(i), ROWS[i])
        for m in range(1, half):
            push(relay_entry(m, i), RELAY[i] + 0.01 * m)
        for m in range(1, nz - 1):
            at(SUMS[i] + 0.01 * m, need, m, i)
    for low, high in GROUPS:
        at(SUMS[high - 1] + 0.2, partial_sums, low, high)
    for u in owns:
        target, d, g, p = u
        if d == 1:
            push(w_entry(u), QUEUE[p] + 0.5 * g)
            done = NEAR[p] + 0.5 * g
        elif d == nz - 1:
            done = LAST[0] + 0.5 * g
        else:
            done = FAR[p] + 3.0 * g + 0.1 * d
            if nz > 4:
                push(w_entry(u), 30.0 + 0.1 * d)
        after = NEXT[p] if d == 1 else NEXT_LAST[0] if d == nz - 1 else NEXT_FAR[p]
        at(done, z_step, u)
        at(done + after[0], f_step, u)
        at(done + after[1], s_step, u)
        at(done + after[1] + (2.0 if done < 90.0 else 1.0), c_step, u)
    queue.sort(key=lambda entry: entry[1])
    previous_time = 0.0
    for n in range(begun, len(queue)):
        previous_time = max(previous_time + 0.001, queue[n][1] - AHEAD, 18.5)
        at(previous_time, pump, n)
    for p in range(wholes):
        at(WHOLE[p], whole_step, p)
        at(WHOLE[p] + 3.0, whole_arrive, p)

    tiles = width // tile
    if nz > 4:
        for p in range(wholes):
            at(26.0, whole_pair(p), "start")
    at(4.0, local_products)
    at(4.1, setup_end)
    if nz == 4:
        for n in range(tiles):
            at(LOCAL[n], local_sums, n, n + 1)
        for p in range(4):
            at(ADDS[p], accumulate, 3, 0, chunks, p * tiles // 4, (p + 1) * tiles // 4)
    else:
        at(4.3, local_sums, 0, tiles)
        for d in range(2, nz):
            at(98.0 + 0.1 * d, accumulate, d, 0, chunks, 0, tiles)
    for load in loads[1:]:
        at(20.0, load.wait)
    for p in range(final_pieces):
        for h, (low, high) in enumerate(SPANS):
            at(FINAL[h][p] if nz == 4 else 99.0 + 0.1 * h + 0.01 * p, final, p, low, high)

    @pl.when(is_inner)
    def _():
        for _, _, body, args in sorted(events, key=lambda event: event[:2]):
            body(*args)

    def pm_copy():
        return remote(carry, partner_map, pm_sem.at[0], pm_sem.at[1], partner)

    pm_copy().start()
    mine = ssq[:, pl.ds(0, 128)]
    for j in range(1, width // 128):
        mine = mine + ssq[:, pl.ds(j * 128, 128)]
    tsums[t] = mine

    def ts_copy(d):
        slot = tsums.at[t]
        return remote(slot, slot, ts_send.at[d - 1], ts_recv.at[d - 1], (z, lax.rem(t + d, nt)))

    def ts_arrival(d):
        slot = tsums.at[lax.rem(t + nt - d, nt)]
        return remote(slot, slot, ts_send.at[d - 1], ts_recv.at[d - 1], partner)

    for d in range(1, nt):
        ts_copy(d).start()

    def m_copy(dq):
        slot = maps.at[chip]
        return remote(
            slot, slot, m_send.at[dq - 1], m_recv.at[dq - 1], (z, 2 * cmod(chip + dq) + core)
        )

    def m_arrival(dq):
        slot = maps.at[cmod(chip - dq)]
        return remote(slot, slot, m_send.at[dq - 1], m_recv.at[dq - 1], partner)

    pm_copy().wait()
    is_second = core == 1
    p_mine, s_mine, p_other, s_other = carry[0], carry[1], partner_map[0], partner_map[1]
    p_late = jnp.where(is_second, p_mine, p_other)
    s_early = jnp.where(is_second, s_other, s_mine)
    s_late = jnp.where(is_second, s_mine, s_other)
    maps[chip, 0] = p_mine * p_other
    maps[chip, 1] = p_late * s_early + s_late
    for dq in range(1, nc):
        m_copy(dq).start()

    @pl.when(is_inner)
    def _():
        for u in owns:
            all_sends(u)
        for entry, _ in queue[max(0, len(queue) - deep):]:
            entry("wait_send")
        for p in range(wholes):
            whole_done(p)
            if nz > 4:
                whole_pair(p)("wait_send")
        for i in range(chunks):
            if nz > 4:
                @pl.when(outward)
                def _():
                    for m in range(1, nz - 1):
                        @pl.when(within(z + s * m))
                        def _():
                            a_copy(1, -m, i).wait_send()

            @pl.when(beside_end)
            def _():
                sum_copy(i).wait_send()

    for d in range(1, nt):
        ts_arrival(d).wait_recv()
    plane = tsums[0]
    for k in range(1, nt):
        plane = plane + tsums[k]
    zsums[z] = plane

    def zs_copy(d):
        slot = zsums.at[z]
        return remote(slot, slot, zs_send.at[d - 1], zs_recv.at[d - 1], (zmod(z + d), t))

    def zs_arrival(d):
        slot = zsums.at[zmod(z - d)]
        return remote(slot, slot, zs_send.at[d - 1], zs_recv.at[d - 1], partner)

    for d in range(1, nz):
        zs_copy(d).start()

    for dq in range(1, nc):
        m_arrival(dq).wait_recv()
    entry = init[...]
    for q in range(nc):
        entry = jnp.where(q < chip, maps[q, 0] * entry + maps[q, 1], entry)
    entry_out[...] = jnp.where(is_second, p_other * entry + s_other, entry)

    for d in range(1, nt):
        ts_copy(d).wait_send()
    for dq in range(1, nc):
        m_copy(dq).wait_send()
    for d in range(1, nz):
        zs_arrival(d).wait_recv()
    whole = zsums[0]
    for k in range(1, nz):
        whole = whole + zsums[k]
    total[...] = whole
    for d in range(1, nz):
        zs_copy(d).wait_send()


def finish(entries, state, prod, entry, total, states, norm, held, out_sem):
    parts = out_sem.shape[0]
    span = state.shape[0] // parts

    def put(n):
        return pltpu.make_async_copy(
            held.at[pl.ds(n * span, span)], states.at[pl.ds(n * span, span)], out_sem.at[n]
        )

    for n in range(parts):
        @pl.loop(n * span, (n + 1) * span)
        def _(q):
            held[q] = prod[q] * entry[...] + state[q]

        put(n).start()
    line = jnp.sum(total[...], axis=0, keepdims=True)
    norm[...] = jnp.sqrt(jnp.sum(line, axis=1, keepdims=True) / entries + 1e-06)
    for n in range(parts):
        put(n).wait()


def local(nz, nt, trajectory, initial, drive_gate, drive_candidate, gate_weight, candidate_weight):
    steps, batch, width = trajectory.shape
    nc = nt // 2
    full = gate_weight.shape[1]
    chunks = 8
    parts = 8
    tile = min(256, width)
    units = len(units_of(nz))
    pieces = 3 if nz == 4 else 4
    ways = 1 if nz == 4 else 2
    entries = trajectory.size * nz * nt
    dma = pltpu.SemaphoreType.DMA
    vmem = pl.BlockSpec(memory_space=pltpu.VMEM)
    hbm = pl.BlockSpec(memory_space=pltpu.HBM)
    block = (steps, batch, width)
    state, prod, entry, total = pl.pallas_call(
        functools.partial(kernel, nz, nt, chunks, tile),
        out_shape=(
            pltpu.VMEM(block, F32),
            pltpu.VMEM(block, F32),
            pltpu.VMEM((batch, width), F32),
            pltpu.VMEM((batch, 128), F32),
        ),
        in_specs=[hbm, vmem, hbm, hbm, hbm, hbm],
        out_specs=(vmem, vmem, vmem, vmem),
        scratch_shapes=[
            pltpu.VMEM((steps + 1, batch, width), F32),
            pltpu.VMEM(block, BF16),
            pltpu.VMEM(block, BF16),
            pltpu.VMEM((2, 2, full, width), BF16),
            pltpu.VMEM((steps * batch, full), BF16),
            pltpu.VMEM((2, steps * batch, width), F32),
            pltpu.VMEM((2, steps * batch, width), F32),
            pltpu.VMEM((2, steps * batch, width), BF16),
            pltpu.VMEM((2, batch, width), F32),
            pltpu.VMEM((2, batch, width), F32),
            pltpu.VMEM((batch, width), F32),
            pltpu.VMEM((2, batch, width), F32),
            pltpu.VMEM((nc, 2, batch, width), F32),
            pltpu.VMEM((nt, batch, 128), F32),
            pltpu.VMEM((nz, batch, 128), F32),
            dma((3,)),
            dma((2, 2)),
            dma((2, pieces)),
            dma((pieces,)),
            dma((pieces,)),
            dma((pieces,)),
            dma((ways, units)),
            dma((units,)),
            dma((units,)),
            dma((units,)),
            dma((units,)),
            dma((units,)),
            dma((ways, nz // 2 if ways == 1 else nz, chunks)),
            dma((nz, chunks)),
            dma((chunks,)),
            dma((chunks,)),
            dma((2,)),
            dma((2,)),
            dma((nc - 1,)),
            dma((nc - 1,)),
            dma((nt - 1,)),
            dma((nt - 1,)),
            dma((nz - 1,)),
            dma((nz - 1,)),
        ],
        compiler_params=pltpu.CompilerParams(
            collective_id=0, has_side_effects=True, vmem_limit_bytes=56 * 2**20
        ),
    )(*(
        pltpu.with_memory_space_constraint(x, pltpu.HBM) if x.ndim == 3 or x.shape[1] == full else x
        for x in (trajectory, initial, drive_gate, drive_candidate, gate_weight, candidate_weight)
    ))
    states, norm = pl.pallas_call(
        functools.partial(finish, entries),
        out_shape=(jax.ShapeDtypeStruct(block, F32), jax.ShapeDtypeStruct((1, 1), F32)),
        in_specs=[vmem, vmem, vmem, vmem],
        out_specs=(hbm, vmem),
        scratch_shapes=[pltpu.VMEM(block, F32), dma((parts,))],
        compiler_params=pltpu.CompilerParams(vmem_limit_bytes=8 * 2**20),
    )(state, prod, entry, total)
    return (states, norm.reshape(()))


def solution(mesh):
    placed = (
        P("tm", None, "chan"),
        P(None, "chan"),
        P("tm", None, "chan"),
        P("tm", None, "chan"),
        P("chan", None),
        P("chan", None),
    )
    body = functools.partial(local, mesh.shape["chan"], mesh.shape["tm"])
    return jax.shard_map(
        body, mesh=mesh, in_specs=placed, out_specs=(P("tm", None, "chan"), P()), check_vma=False
    )
```

```python
import functools

import jax
import jax.numpy as jnp
from jax import lax
from jax.experimental import pallas as pl
from jax.experimental.pallas import tpu as pltpu
from jax.sharding import PartitionSpec as P

MESH = pl.DeviceIdType.MESH
BF16 = jnp.bfloat16
F32 = jnp.float32

PACED = [0.0, 9.0, 13.65, 17.0]
FIRST = [10.0, 15.5, 20.5, 26.0]
FIRST_F = [13.5, 19.0, 27.0, 36.0]
FIRST_S = [18.0, 26.0, 34.5, 43.0]
LOCAL = [25.5, 34.4, 36.5, 42.9]
AHEAD = 12.0
AFTER = 3.0
ROWS = [28.0, 36.0, 40.0, 48.0, 59.0, 64.0, 72.0, 77.0]
RELAY = [30.5, 38.0, 43.0, 51.0, 61.5, 66.0, 74.0, 80.0]
QUEUE = [33.0, 46.0, 63.0, 75.5]
SUMS = [47.0, 47.1, 58.5, 66.5, 71.5, 77.5, 81.0, 88.4]
GROUPS = [(0, 2), (2, 3), (3, 4), (4, 5), (5, 6), (6, 7), (7, 8)]
NEAR = [42.5, 53.0, 74.3, 83.0]
NEXT = [(8.0, 12.0), (8.0, 12.0), (5.2, 8.0), (4.8, 6.2)]
FAR = [45.5, 63.0]
NEXT_FAR = [(9.0, 14.5), (6.0, 12.0)]
LAST = [71.0, 71.1]
NEXT_LAST = [(7.0, 12.5), (7.1, 12.6)]
WHOLE = [70.5, 76.9, 84.3, 84.4]
ADDS = [74.0, 80.0, 87.3, 87.35]
SPANS = [(0, 4), (4, 6), (6, 8)]
FINAL = [[74.2, 80.1, 87.5, 96.2], [80.2, 80.3, 89.75, 96.3], [89.8, 89.9, 90.0, 96.4]]


def units_of(nz):
    near, far = (4, 2) if nz <= 4 else (1, 1)
    units = [(1, d, g, p, near) for p in range(near) for g in range(2) for d in range(1, nz - 1)]
    for d in range(1, nz - 1):
        pieces = near if d == 1 else far
        units += [(0, d, g, p, pieces) for p in range(pieces) for g in range(2)]
    if nz <= 4:
        units += [(0, nz - 1, g, p, near) for p in range(near // 2, near) for g in range(2)]
    return units


def split(count):
    rows = 1
    while rows * rows * 4 <= count:
        rows *= 2
    return rows, count // rows


def kernel(
    nz, nt, chunks, tile,
    traj_in, init, drive_g_in, drive_c_in, gate_w, cand_w,
    state, prod, entry_out, total,
    guess_buf, drive_g, drive_c, wbuf, abuf, acc, end_acc, sbuf,
    diag, carry, ssq, partner_map, maps, tsums, zsums,
    load_sem, local_sem, wr_send, wr_recv, cr_send, cr_recv, wz_send, wz_recv, spread_send, f_recv, s_recv, c_recv,
    a_send, a_recv, sum_send, sum_recv, row_sem, pm_sem, m_send, m_recv, ts_send, ts_recv, zs_send, zs_recv,
):
    z = lax.axis_index("chan")
    t = lax.axis_index("tm")
    steps, batch, width = traj_in.shape
    nc = nt // 2
    na, nb = split(nc)
    chip = lax.div(t, 2)
    core = lax.rem(t, 2)
    chip_a = lax.div(chip, nb)
    chip_b = lax.rem(chip, nb)
    partner = (z, t + 1 - 2 * core)
    part = width // nt
    weights = (gate_w, cand_w)
    rows = steps * batch // chunks
    cuts = [(i * rows, rows) for i in range(chunks)]
    half = nz // 2
    units = units_of(nz)
    index = {u[:4]: n for n, u in enumerate(units)}
    count = {u[:4]: u[4] for u in units}
    lower = z < half
    s = jnp.where(lower, 1, -1)
    is_end = jnp.logical_or(z == 0, z == nz - 1)
    is_inner = jnp.logical_not(is_end)
    beside_end = jnp.logical_or(z == 1, z == nz - 2)
    end = jnp.where(lower, 0, nz - 1)

    def remote(src, dst, send, recv, device):
        return pltpu.make_async_remote_copy(
            src_ref=src, dst_ref=dst, send_sem=send, recv_sem=recv,
            device_id=device, device_id_type=MESH,
        )

    def zmod(v):
        return lax.rem(v + 2 * nz, nz)

    def cmod(v):
        return lax.rem(v + 2 * nc, nc)

    def plane_cols(k):
        return pl.ds(pl.multiple_of(k * width, 128), width)

    def piece_cols(p, pieces):
        return pl.ds(p * (width // pieces), width // pieces)

    def chip_at(g, fast, slow):
        da, db = (slow, fast) if g == 0 else (fast, slow)
        return lax.rem(chip_a + da + na, na) * nb + lax.rem(chip_b + db + nb, nb)

    def extent(g):
        return (nb, na) if g == 0 else (na, nb)

    loads = [
        pltpu.make_async_copy(traj_in, guess_buf.at[pl.ds(1, steps)], load_sem.at[0]),
        pltpu.make_async_copy(drive_g_in, drive_g, load_sem.at[1]),
        pltpu.make_async_copy(drive_c_in, drive_c, load_sem.at[2]),
    ]
    for load in loads:
        load.start()

    barrier = pltpu.get_barrier_semaphore()
    for d in range(1, nz):
        pl.semaphore_signal(barrier, inc=1, device_id=(zmod(z + d), t), device_id_type=MESH)
    for d in range(1, nt):
        pl.semaphore_signal(barrier, inc=1, device_id=(z, lax.rem(t + d, nt)), device_id_type=MESH)
    pl.semaphore_wait(barrier, nz - 1 + nt - 1)

    def row_copy():
        return remote(
            traj_in.at[steps - 1], guess_buf.at[0], row_sem.at[0], row_sem.at[1], (z, lax.rem(t + 1, nt))
        )

    def w_slot(target, g, k, p, pieces, c):
        first = pl.multiple_of(k * width + (2 * c + core) * part, 16)
        return wbuf.at[target, g, pl.ds(first, part), piece_cols(p, pieces)]

    def w_send(unit, side, method):
        target, d, g, p = unit
        n, pieces = index[unit], count[unit]
        j = zmod(z - d) if side == 0 else zmod(z + d)
        if target == 1:
            valid = j == (1 if side == 0 else nz - 2)
            out = jnp.where(side == 0, 0, nz - 1)
        elif side == 0:
            valid = jnp.logical_and(j >= 1, j < half)
            out = j
        else:
            valid = jnp.logical_and(j >= half, j <= nz - 2)
            out = j

        @pl.when(valid)
        def _():
            step = width // pieces
            src = weights[g].at[
                pl.ds(pl.multiple_of(t * part, 16), part),
                pl.ds(pl.multiple_of(out * width + p * step, 128), step),
            ]
            copy = remote(
                src, w_slot(target, g, z, p, pieces, chip), wz_send.at[side % wz_send.shape[0], n], wz_recv.at[n], (j, t)
            )
            getattr(copy, method)()

    def w_pair(unit):
        def act(method):
            for side in range(2):
                w_send(unit, side, method)

        return act

    wholes = wr_recv.shape[0]
    whole_pieces = 4

    def whole_slot(g, k, p):
        return wbuf.at[0, g, plane_cols(k), piece_cols(p, whole_pieces)]

    def whole_pair(p):
        def act(method):
            for side in range(2):
                j = zmod(z + 1) if side == 0 else zmod(z - 1)
                valid = jnp.logical_and(j >= 1, j < half) if side == 0 else jnp.logical_and(j >= half, j <= nz - 2)
                step = width // whole_pieces
                for g in range(2):
                    @pl.when(jnp.logical_and(valid, core == g))
                    def _():
                        src = weights[g].at[:, pl.ds(pl.multiple_of(j * width + p * step, 128), step)]
                        copy = remote(src, whole_slot(g, z, p), wr_send.at[side, p], wr_recv.at[p], (j, t))
                        getattr(copy, method)()

        return act

    def run(entries, depth):
        for n, entry in enumerate(entries):
            if n >= depth:
                entries[n - depth]("wait_send")
            entry("start")
        for entry in entries[max(0, len(entries) - depth):]:
            entry("wait_send")

    row_copy().start()
    ahead = 4
    deep = 64
    first_units = [u[:4] for u in units if u[0] == 1]
    groups = max(u[3] for u in first_units) + 1

    def paced_weights(p):
        first_weights(p, p + 1)

    def first_weights(low, high):
        for u in first_units:
            if low <= u[3] < high:
                w_pair(u)("start")

    first_weights(0, 1)

    def own_copy(target, g):
        out = z if target == 0 else end
        return pltpu.make_async_copy(
            weights[g].at[:, plane_cols(out)],
            wbuf.at[target, g, plane_cols(z), :],
            local_sem.at[target, g],
        )

    for g in range(2):
        own_copy(0, g).start()

    @pl.when(is_inner)
    def _():
        for g in range(2):
            @pl.when(beside_end)
            def _():
                own_copy(1, g).start()

    for g in range(2):
        own_copy(0, g).wait()
        for j in range(width // 128):
            block = wbuf[0, g, pl.ds(pl.multiple_of(z * width + j * 128, 128), 128), pl.ds(j * 128, 128)]
            eye = lax.broadcasted_iota(jnp.int32, (128, 128), 0) == lax.broadcasted_iota(
                jnp.int32, (128, 128), 1
            )
            line = jnp.sum(jnp.where(eye, block.astype(F32), 0.0), axis=0, keepdims=True)
            diag[g, :, pl.ds(j * 128, 128)] = jnp.broadcast_to(line, (batch, 128))
    loads[0].wait()

    @pl.loop(1, steps // 2)
    def _(j):
        pair = guess_buf[pl.ds(2 * j, 2)].reshape(2 * batch, width)
        abuf[pl.ds(pl.multiple_of(j * 2 * batch, 16), 2 * batch), plane_cols(z)] = pair.astype(BF16)

    row_copy().wait()

    @pl.when(t == 0)
    def _():
        guess_buf[0] = init[...]

    abuf[pl.ds(0, 2 * batch), plane_cols(z)] = guess_buf[pl.ds(0, 2)].reshape(2 * batch, width).astype(BF16)

    def a_copy(way, m, i):
        k = z - s * m
        slot = abuf.at[pl.ds(*cuts[i]), plane_cols(k)]
        to = z + s if way == 0 else z - s
        return remote(slot, slot, a_send.at[way, min(abs(m), a_send.shape[1] - 1), i], a_recv.at[k, i], (to, t))

    def sum_copy(i, h):
        slot = sbuf.at[:, pl.ds(*cuts[i]), piece_cols(h, 2)]
        return remote(slot, slot, sum_send.at[2 * i + h], sum_recv.at[2 * i + h], (z - s, t))

    carry[0] = jnp.ones((batch, width), F32)
    carry[1] = jnp.zeros((batch, width), F32)
    ssq[...] = jnp.zeros((batch, width), F32)

    def local_products():
        @pl.loop(0, width // tile)
        def _(n):
            cols = pl.ds(pl.multiple_of(n * tile, tile), tile)
            for g in range(2):
                acc[g, :, cols] = jnp.dot(
                    abuf[:, plane_cols(z)], wbuf[0, g, plane_cols(z), cols], preferred_element_type=F32
                )

    def accumulate(d, low, high, first, last):
        k = zmod(z + s * d)
        span = pl.ds(low * rows, (high - low) * rows)

        @pl.loop(first, last)
        def _(n):
            cols = pl.ds(pl.multiple_of(n * tile, tile), tile)
            for g in range(2):
                acc[g, span, cols] += jnp.dot(
                    abuf[span, plane_cols(k)], wbuf[0, g, plane_cols(k), cols], preferred_element_type=F32
                )

    def gates(first, length, cols, wide, gate_pre, cand_pre):
        shape = (length, batch, wide)
        span = pl.ds(first, length)
        gate_pre = gate_pre.reshape(shape) + drive_g[span, :, cols].astype(F32)
        cand_pre = cand_pre.reshape(shape) + drive_c[span, :, cols].astype(F32)
        guess = guess_buf[pl.ds(first + 1, length), :, cols]
        previous = guess_buf[span, :, cols]
        update = jax.nn.sigmoid(gate_pre)
        candidate = jnp.tanh(cand_pre)
        keep = 1.0 - update
        mapped = keep * previous + update * candidate
        jacobian = (
            keep
            + update * keep * (candidate - previous) * diag[0, :, cols][None]
            + update * (1.0 - candidate * candidate) * diag[1, :, cols][None]
        )
        offset = mapped - jacobian * previous
        missing = guess - mapped
        ssq[:, cols] += jnp.sum(missing * missing, axis=0)
        product = carry[0, :, cols]
        value = carry[1, :, cols]
        for q in range(length):
            product = jacobian[q] * product
            value = jacobian[q] * value + offset[q]
            prod[first + q, :, cols] = product
            state[first + q, :, cols] = value
        carry[0, :, cols] = product
        carry[1, :, cols] = value

    final_pieces = count[(0, 1, 0, 0)]

    @pl.when(is_end)
    def _():
        def a_entry(i):
            return lambda method: getattr(a_copy(0, 0, i), method)()

        owns = [u[:4] for u in units if u[0] == 0 and half <= u[1] < nz - 1]
        lasts = [u[:4] for u in units if u[0] == 0 and u[1] == nz - 1]
        some = (len(owns) + 1) // 2
        whole = [whole_pair(p) for p in range(wholes)]
        local_products()
        for p in range(1, groups):
            paced_weights(p)
            for u in first_units:
                if u[3] == p - 1:
                    w_pair(u)("wait_send")
        run([a_entry(i) for i in range(chunks // 2)], ahead)
        run([w_pair(u) for u in owns[:some]], ahead)
        run([a_entry(i) for i in range(chunks // 2, len(cuts))], ahead)
        whole[0]("start")
        run([w_pair(u) for u in owns[some:] + lasts], ahead)
        for p in range(1, wholes):
            whole[p]("start")
        for p in range(wholes):
            whole[p]("wait_send")
        for u in first_units:
            if u[3] == groups - 1:
                w_pair(u)("wait_send")
        for load in loads[1:]:
            load.wait()
        half_tiles = width // tile // 2
        for i, h in [(i, h) for i in range(len(cuts)) for h in range(2)]:
            sum_copy(i, h).wait_recv()

            @pl.loop(h * half_tiles, (h + 1) * half_tiles)
            def _(n):
                cols = pl.ds(pl.multiple_of(n * tile, tile), tile)
                span = pl.ds(*cuts[i])
                gates(
                    cuts[i][0] // batch, cuts[i][1] // batch, cols, tile,
                    acc[0, span, cols] + sbuf[0, span, cols].astype(F32),
                    acc[1, span, cols] + sbuf[1, span, cols].astype(F32),
                )

    def spread(unit, arrive, df, ds, device):
        target, d, g, p = unit
        n = index[unit]
        slot = w_slot(target, g, zmod(z + s * d), p, count[unit], chip_at(g, -df, -ds))
        return remote(slot, slot, spread_send.at[n], arrive.at[n], device)

    def f_copy(unit, df):
        return spread(unit, f_recv, 0, 0, (z, 2 * chip_at(unit[2], df, 0) + core))

    def s_copy(unit, df, ds):
        return spread(unit, s_recv, df, 0, (z, 2 * chip_at(unit[2], 0, ds) + core))

    def c_copy(unit, df, ds):
        return spread(unit, c_recv, df, ds, partner)

    def parts_of(unit, arrive, parts):
        target, d, g, p = unit
        n = index[unit]
        slot = wbuf.at[target, g, pl.ds(0, parts * part), piece_cols(p, count[unit])]
        return remote(slot, slot, spread_send.at[n], arrive.at[n], partner)

    def guarded(unit, body):
        if unit[0] == 1 and nz > 4:
            pl.when(beside_end)(body)
        else:
            body()

    def z_step(unit):
        def body():
            target, d, g, p = unit
            n = index[unit]
            nf, ns = extent(g)
            slot = w_slot(target, g, zmod(z + s * d), p, count[unit], chip)
            remote(slot, slot, wz_send.at[0, n], wz_recv.at[n], partner).wait_recv()
            for df in range(1, nf):
                f_copy(unit, df).start()
            for ds in range(1, ns):
                s_copy(unit, 0, ds).start()
            c_copy(unit, 0, 0).start()

        guarded(unit, body)

    def f_step(unit):
        def body():
            nf, ns = extent(unit[2])
            if nf > 1:
                parts_of(unit, f_recv, nf - 1).wait_recv()
            for df in range(1, nf):
                for ds in range(1, ns):
                    s_copy(unit, df, ds).start()
                c_copy(unit, df, 0).start()

        guarded(unit, body)

    def s_step(unit):
        def body():
            nf, ns = extent(unit[2])
            if ns > 1:
                parts_of(unit, s_recv, nf * (ns - 1)).wait_recv()
            for df in range(nf):
                for ds in range(1, ns):
                    c_copy(unit, df, ds).start()

        guarded(unit, body)

    def c_step(unit):
        def body():
            nf, ns = extent(unit[2])
            parts_of(unit, c_recv, nf * ns).wait_recv()

        guarded(unit, body)

    def all_sends(unit):
        def body():
            nf, ns = extent(unit[2])
            parts_of(unit, c_recv, nf - 1 + nf * (ns - 1) + nf * ns).wait_send()

        guarded(unit, body)

    def within(k):
        return jnp.logical_and(k >= 0, k < nz)

    outward = jnp.logical_and(z - s >= 1, z - s <= nz - 2)

    def need(m, i):
        @pl.when(within(z + s * m))
        def _():
            a_copy(0, -m, i).wait_recv()
            if nz > 4:
                @pl.when(outward)
                def _():
                    a_copy(1, -m, i).start()

    def local_sums(first, last):
        def body():
            @pl.loop(first, last)
            def _(n):
                cols = pl.ds(pl.multiple_of(n * tile, tile), tile)
                for g in range(2):
                    end_acc[g, :, cols] = jnp.dot(
                        abuf[:, plane_cols(z)], wbuf[1, g, plane_cols(z), cols], preferred_element_type=F32
                    )

        if nz > 4:
            pl.when(beside_end)(body)
        else:
            body()

    def partial_sums(low, high):
        def body():
            depth = (nz - 2) * width
            first = pl.multiple_of(jnp.where(lower, 2 * width, 0), 128)
            span = pl.ds(cuts[low][0], sum(cut[1] for cut in cuts[low:high]))

            half_tiles = width // tile // 2
            for h in range(2):
                @pl.loop(h * half_tiles, (h + 1) * half_tiles)
                def _(n):
                    cols = pl.ds(pl.multiple_of(n * tile, tile), tile)
                    lhs = abuf[span, pl.ds(first, depth)]
                    for g in range(2):
                        sbuf[g, span, cols] = (
                            end_acc[g, span, cols]
                            + jnp.dot(lhs, wbuf[1, g, pl.ds(first, depth), cols], preferred_element_type=F32)
                        ).astype(BF16)

                for i in range(low, high):
                    sum_copy(i, h).start()

        if nz > 4:
            pl.when(beside_end)(body)
        else:
            body()

    def final(p, low, high):
        blocks = [zmod(z + s * d) for d in ((1, 2) if nz == 4 else (1,))]
        wide = width // final_pieces
        long = rows * 2

        @pl.loop(low // 2, high // 2)
        def _(r):
            span = pl.ds(pl.multiple_of(r * long, long), long)
            for n in range(wide // min(tile, wide)):
                step = min(tile, wide)
                cols = pl.ds(p * wide + n * step, step)
                pre = []
                for g in range(2):
                    sums = acc[g, span, cols]
                    for k in blocks:
                        sums += jnp.dot(
                            abuf[span, plane_cols(k)], wbuf[0, g, plane_cols(k), cols],
                            preferred_element_type=F32,
                        )
                    pre.append(sums)
                gates(r * (long // batch), long // batch, cols, step, *pre)

    def setup_end():
        def body():
            for g in range(2):
                own_copy(1, g).wait()

        if nz > 4:
            pl.when(beside_end)(body)
        else:
            body()

    def whole_step(p):
        k = zmod(z - s)
        for g in range(2):
            @pl.when(core == g)
            def _():
                slot = whole_slot(g, k, p)
                remote(slot, slot, wr_send.at[0, p], wr_recv.at[p], partner).wait_recv()
                remote(slot, slot, cr_send.at[p], cr_recv.at[p], partner).start()

    def whole_arrive(p):
        slot = whole_slot(0, zmod(z - s), p)
        remote(slot, slot, cr_send.at[p], cr_recv.at[p], partner).wait_recv()

    def whole_done(p):
        slot = whole_slot(0, zmod(z - s), p)
        remote(slot, slot, cr_send.at[p], cr_recv.at[p], partner).wait_send()

    events = []

    def at(time, body, *args):
        events.append((time, len(events), body, args))

    def w_entry(unit):
        return w_pair(unit)

    def rows_entry(i):
        def act(method):
            getattr(a_copy(0, 0, i), method)()
            if nz > 4:
                @pl.when(outward)
                def _():
                    getattr(a_copy(1, 0, i), method)()

        return act

    def relay_entry(m, i):
        def act(method):
            @pl.when(within(z - s * m))
            def _():
                if method == "start":
                    a_copy(0, m, i).wait_recv()
                getattr(a_copy(0, m, i), method)()

        return act

    queue = []

    def push(entry, done):
        queue.append((entry, done))

    def pump(n):
        if n >= deep:
            queue[n - deep][0]("wait_send")
        queue[n][0]("start")

    ends = [u[:4] for u in units if u[0] == 1]
    owns = [u[:4] for u in units if u[0] == 0]
    for u in ends:
        target, d, g, p = u
        e = 4 * p // groups if groups >= 4 else p
        at(FIRST[e] + 0.1 * d, z_step, u)
        at(FIRST_F[e] + 0.1 * d, f_step, u)
        at(FIRST_S[e] + 0.1 * d, s_step, u)
        at(SUMS[0] - 0.5, c_step, u)
        at(SUMS[0] + 10.0, all_sends, u)
    begun = 0
    for p in range(1, groups):
        at(PACED[p % 4], paced_weights, p)

    def last_paced():
        for u in first_units:
            w_pair(u)("wait_send")

    at(60.0, last_paced)
    for i in range(len(cuts)):
        push(rows_entry(i), ROWS[i])
        for m in range(1, half):
            push(relay_entry(m, i), RELAY[i] + 0.01 * m)
        for m in range(1, nz - 1):
            at(SUMS[i] + 0.01 * m, need, m, i)
    for low, high in GROUPS:
        at(SUMS[high - 1] + 0.2, partial_sums, low, high)
    for u in owns:
        target, d, g, p = u
        if d == 1:
            push(w_entry(u), QUEUE[p] + 0.5 * g)
            done = NEAR[p] + 0.5 * g
        elif d == nz - 1:
            done = LAST[p - 2] + 0.5 * g
        else:
            done = FAR[p] + 3.0 * g + 0.1 * d
            if nz > 4:
                push(w_entry(u), 30.0 + 0.1 * d)
        after = NEXT[p] if d == 1 else NEXT_LAST[p - 2] if d == nz - 1 else NEXT_FAR[p]
        at(done, z_step, u)
        at(done + after[0], f_step, u)
        at(done + after[1], s_step, u)
        at(done + after[1] + AFTER, c_step, u)
    queue.sort(key=lambda entry: entry[1])
    previous_time = 0.0
    for n in range(begun, len(queue)):
        previous_time = max(previous_time + 0.001, queue[n][1] - AHEAD, 18.5)
        at(previous_time, pump, n)
    for p in range(wholes):
        at(WHOLE[p], whole_step, p)
        at(WHOLE[p] + 3.0, whole_arrive, p)

    tiles = width // tile
    if nz > 4:
        for p in range(wholes):
            at(26.0, whole_pair(p), "start")
    at(4.0, local_products)
    at(4.1, setup_end)
    if nz == 4:
        for n in range(tiles):
            at(LOCAL[n], local_sums, n, n + 1)
        for p in range(4):
            at(ADDS[p], accumulate, 3, 0, chunks, p * tiles // 4, (p + 1) * tiles // 4)
    else:
        at(4.3, local_sums, 0, tiles)
        for d in range(2, nz):
            at(98.0 + 0.1 * d, accumulate, d, 0, chunks, 0, tiles)
    for load in loads[1:]:
        at(20.0, load.wait)
    for p in range(final_pieces):
        for h, (low, high) in enumerate(SPANS):
            at(FINAL[h][p] if nz == 4 else 99.0 + 0.1 * h + 0.01 * p, final, p, low, high)

    @pl.when(is_inner)
    def _():
        for _, _, body, args in sorted(events, key=lambda event: event[:2]):
            body(*args)

    def pm_copy():
        return remote(carry, partner_map, pm_sem.at[0], pm_sem.at[1], partner)

    pm_copy().start()
    mine = ssq[:, pl.ds(0, 128)]
    for j in range(1, width // 128):
        mine = mine + ssq[:, pl.ds(j * 128, 128)]
    tsums[t] = mine

    def ts_copy(d):
        slot = tsums.at[t]
        return remote(slot, slot, ts_send.at[0], ts_recv.at[0], (z, lax.rem(t + d, nt)))

    def ts_all():
        slot = tsums.at[pl.ds(0, nt - 1)]
        return remote(slot, slot, ts_send.at[0], ts_recv.at[0], partner)

    for d in range(1, nt):
        ts_copy(d).start()

    def m_copy(dq):
        slot = maps.at[chip]
        return remote(
            slot, slot, m_send.at[0], m_recv.at[0], (z, 2 * cmod(chip + dq) + core)
        )

    def m_all():
        slot = maps.at[pl.ds(0, nc - 1)]
        return remote(slot, slot, m_send.at[0], m_recv.at[0], partner)

    pm_copy().wait()
    is_second = core == 1
    p_mine, s_mine, p_other, s_other = carry[0], carry[1], partner_map[0], partner_map[1]
    p_late = jnp.where(is_second, p_mine, p_other)
    s_early = jnp.where(is_second, s_other, s_mine)
    s_late = jnp.where(is_second, s_mine, s_other)
    maps[chip, 0] = p_mine * p_other
    maps[chip, 1] = p_late * s_early + s_late
    for dq in range(1, nc):
        m_copy(dq).start()

    @pl.when(is_inner)
    def _():
        for u in owns:
            all_sends(u)
        for entry, _ in queue[max(0, len(queue) - deep):]:
            entry("wait_send")
        for p in range(wholes):
            whole_done(p)
            if nz > 4:
                whole_pair(p)("wait_send")
        for i in range(len(cuts)):
            if nz > 4:
                @pl.when(outward)
                def _():
                    for m in range(1, nz - 1):
                        @pl.when(within(z + s * m))
                        def _():
                            a_copy(1, -m, i).wait_send()

            @pl.when(beside_end)
            def _():
                for h in range(2):
                    sum_copy(i, h).wait_send()

    ts_all().wait_recv()
    plane = tsums[0]
    for k in range(1, nt):
        plane = plane + tsums[k]
    zsums[z] = plane

    def zs_copy(d):
        slot = zsums.at[z]
        return remote(slot, slot, zs_send.at[0], zs_recv.at[0], (zmod(z + d), t))

    def zs_all():
        slot = zsums.at[pl.ds(0, nz - 1)]
        return remote(slot, slot, zs_send.at[0], zs_recv.at[0], partner)

    for d in range(1, nz):
        zs_copy(d).start()

    m_all().wait_recv()
    entry = init[...]
    for q in range(nc):
        entry = jnp.where(q < chip, maps[q, 0] * entry + maps[q, 1], entry)
    entry_out[...] = jnp.where(is_second, p_other * entry + s_other, entry)

    ts_all().wait_send()
    m_all().wait_send()
    zs_all().wait_recv()
    whole = zsums[0]
    for k in range(1, nz):
        whole = whole + zsums[k]
    total[...] = whole
    zs_all().wait_send()


def finish(entries, state, prod, entry, total, states, norm, held, out_sem):
    parts = out_sem.shape[0]
    span = state.shape[0] // parts

    def put(n):
        return pltpu.make_async_copy(
            held.at[pl.ds(n * span, span)], states.at[pl.ds(n * span, span)], out_sem.at[n]
        )

    for n in range(parts):
        @pl.loop(n * span, (n + 1) * span)
        def _(q):
            held[q] = prod[q] * entry[...] + state[q]

        put(n).start()
    line = jnp.sum(total[...], axis=0, keepdims=True)
    norm[...] = jnp.sqrt(jnp.sum(line, axis=1, keepdims=True) / entries + 1e-06)
    for n in range(parts):
        put(n).wait()


def local(nz, nt, trajectory, initial, drive_gate, drive_candidate, gate_weight, candidate_weight):
    steps, batch, width = trajectory.shape
    nc = nt // 2
    full = gate_weight.shape[1]
    chunks = 8
    parts = 8
    tile = min(256, width)
    units = len(units_of(nz))
    pieces = 2 if nz == 4 else 4
    ways = 1 if nz == 4 else 2
    entries = trajectory.size * nz * nt
    dma = pltpu.SemaphoreType.DMA
    vmem = pl.BlockSpec(memory_space=pltpu.VMEM)
    hbm = pl.BlockSpec(memory_space=pltpu.HBM)
    block = (steps, batch, width)
    state, prod, entry, total = pl.pallas_call(
        functools.partial(kernel, nz, nt, chunks, tile),
        out_shape=(
            pltpu.VMEM(block, F32),
            pltpu.VMEM(block, F32),
            pltpu.VMEM((batch, width), F32),
            pltpu.VMEM((batch, 128), F32),
        ),
        in_specs=[hbm, vmem, hbm, hbm, hbm, hbm],
        out_specs=(vmem, vmem, vmem, vmem),
        scratch_shapes=[
            pltpu.VMEM((steps + 1, batch, width), F32),
            pltpu.VMEM(block, BF16),
            pltpu.VMEM(block, BF16),
            pltpu.VMEM((2, 2, full, width), BF16),
            pltpu.VMEM((steps * batch, full), BF16),
            pltpu.VMEM((2, steps * batch, width), F32),
            pltpu.VMEM((2, steps * batch, width), F32),
            pltpu.VMEM((2, steps * batch, width), BF16),
            pltpu.VMEM((2, batch, width), F32),
            pltpu.VMEM((2, batch, width), F32),
            pltpu.VMEM((batch, width), F32),
            pltpu.VMEM((2, batch, width), F32),
            pltpu.VMEM((nc, 2, batch, width), F32),
            pltpu.VMEM((nt, batch, 128), F32),
            pltpu.VMEM((nz, batch, 128), F32),
            dma((3,)),
            dma((2, 2)),
            dma((2, pieces)),
            dma((pieces,)),
            dma((pieces,)),
            dma((pieces,)),
            dma((ways, units)),
            dma((units,)),
            dma((units,)),
            dma((units,)),
            dma((units,)),
            dma((units,)),
            dma((ways, nz // 2 if ways == 1 else nz, chunks)),
            dma((nz, chunks)),
            dma((2 * chunks,)),
            dma((2 * chunks,)),
            dma((2,)),
            dma((2,)),
            dma((1,)),
            dma((1,)),
            dma((1,)),
            dma((1,)),
            dma((1,)),
            dma((1,)),
        ],
        compiler_params=pltpu.CompilerParams(
            collective_id=0, has_side_effects=True, vmem_limit_bytes=56 * 2**20
        ),
    )(*(
        pltpu.with_memory_space_constraint(x, pltpu.HBM) if x.ndim == 3 or x.shape[1] == full else x
        for x in (trajectory, initial, drive_gate, drive_candidate, gate_weight, candidate_weight)
    ))
    states, norm = pl.pallas_call(
        functools.partial(finish, entries),
        out_shape=(jax.ShapeDtypeStruct(block, F32), jax.ShapeDtypeStruct((1, 1), F32)),
        in_specs=[vmem, vmem, vmem, vmem],
        out_specs=(hbm, vmem),
        scratch_shapes=[pltpu.VMEM(block, F32), dma((parts,))],
        compiler_params=pltpu.CompilerParams(vmem_limit_bytes=8 * 2**20),
    )(state, prod, entry, total)
    return (states, norm.reshape(()))


def solution(mesh):
    placed = (
        P("tm", None, "chan"),
        P(None, "chan"),
        P("tm", None, "chan"),
        P("tm", None, "chan"),
        P("chan", None),
        P("chan", None),
    )
    body = functools.partial(local, mesh.shape["chan"], mesh.shape["tm"])
    return jax.shard_map(
        body, mesh=mesh, in_specs=placed, out_specs=(P("tm", None, "chan"), P()), check_vma=False
    )
```
